32 devices in a mesh: gx: 8 (over y, x, core), gy: 4 (over z).
Axes of the slice: x: 2, y: 2, z: 4, core: 2. Of those that a mesh axis runs over, the one named last changes fastest.
Arguments:
- features: bfloat16 [8, 4, 128, 128], P('gx', 'gy'), may hold values from -6 to 6
- offsets: float32 [8, 4, 3, 128], P('gx', 'gy'), may hold values from 0 to 1
- counts: int32 [8, 4, 4], P('gx', 'gy'), may hold values from 1 to 32, as said below
- wave_index: int32 [3, 512], replicated, may hold values from -5 to 5, as said below
- screening: float32 [2, 128], replicated, may hold values from 1 to 8
- charge_weight: bfloat16 [2, 128, 128], replicated, may hold values from -0.5 to 0.5
- ewald_weight: bfloat16 [2, 128, 128], replicated, may hold values from -0.5 to 0.5
- input_weight: bfloat16 [2, 128, 128], replicated, may hold values from -0.5 to 0.5
- filter_weight: bfloat16 [2, 128, 128], replicated, may hold values from -0.5 to 0.5
- middle_weight: bfloat16 [2, 128, 128], replicated, may hold values from -0.5 to 0.5
- output_weight: bfloat16 [2, 128, 128], replicated, may hold values from -0.5 to 0.5
Outputs:
- updated: bfloat16 [8, 4, 128, 128], P('gx', 'gy')
The draws below stay inside these ranges and needn't reach their ends.
Inputs may be any that keep to these rules, and one draw needn't show every extreme that they name: `counts`: atoms in a cell; some cell of every draw is full. `wave_index`: integer wave numbers; the 512 vectors are distinct, none is zero, and no two are opposite.
All inputs are finite; a program needn't handle non-finite values.
Results may differ from the reference program's by a relative error of at most 0.007.
Values may be sent and summed in bfloat16 or wider, within the bound.
No kernel may reach another device: no remote copies, remote signals or barrier semaphores. Data moves between devices by JAX's collectives and lax.ppermute only.
A program may use at most 64 MiB of HBM per device.

```python
import math
import jax
import jax.numpy as jnp
from jax import lax

F = 128
RBF = 128
K = 512
A = 32
GZ = 4
CELLS_X = 8
CELLS_Y = 4


def draw_counts(key, part):
    first, second = jax.random.split(jax.random.fold_in(key, 11))
    light = jax.random.randint(first, (CELLS_X, CELLS_Y, GZ), 1, max(A // 8, 1) + 1)
    heavy = jax.random.randint(second, (CELLS_X, CELLS_Y, 1), 0, 8)
    heavy = heavy.at[0, 0, 0].set(0)
    heavy = heavy.at[CELLS_X // 2, 0, 0].set(0)
    filled = jnp.where(heavy == 0, A, light)
    return filled.astype(jnp.int32)


def draw_wave_index(key, part):
    chosen = jax.random.permutation(jax.random.fold_in(key, 23), 665)[:K] + 666
    along_x = chosen // 121 - 5
    along_y = chosen // 11 % 11 - 5
    along_z = chosen % 11 - 5
    return jnp.stack([along_x, along_y, along_z]).astype(jnp.int32)


def level_of(own_key, dims, shards, smallest, top_value):
    def one(dim, parts):
        steps = jax.random.uniform(jax.random.fold_in(jax.random.fold_in(own_key, 6), dim), (parts,), jnp.float32, smallest / len(shards), top_value / len(shards))
        return jnp.repeat(jnp.exp(steps), dims[dim] // parts).reshape((-1,) + (1,) * (len(dims) - dim - 1))

    gain = one(*shards[0])
    for cut in shards[1:]:
        gain = gain * one(*cut)
    return gain


def bell_draw(own_key, extent, spread, limit, cuts=(), kind=jnp.bfloat16):
    gain = level_of(own_key, extent, cuts, -0.22, 0.18) if cuts else 1.0
    entries = jax.random.normal(own_key, extent, jnp.float32) * spread * gain
    return jnp.minimum(jnp.maximum(entries, -limit), limit).astype(kind)


def setup_inputs(seed: int = 0) -> dict:
    keys = jax.random.split(jax.random.key(seed), 12)
    return {
        "features": bell_draw(keys[0], (CELLS_X, CELLS_Y, GZ * A, F), 1.0, 6.0, ((0, 8), (1, 4))),
        "offsets": jnp.clip(1.0 * jax.random.uniform(keys[1], (CELLS_X, CELLS_Y, 3, GZ * A), jnp.float32) ** level_of(keys[1], (CELLS_X, CELLS_Y, 3, GZ * A), ((0, 8), (1, 4)), -0.2, 0.2), 0.0, 1.0),
        "counts": draw_counts(jax.random.fold_in(keys[11], 71), 0),
        "wave_index": draw_wave_index(jax.random.fold_in(keys[11], 71), 0),
        "screening": jnp.clip(jnp.exp(jax.random.uniform(keys[4], (2, F), jnp.float32, math.log(1.0), math.log(8.0))), 1.0, 8.0),
        "charge_weight": bell_draw(keys[5], (2, F, F), F ** -0.5, 0.5),
        "ewald_weight": bell_draw(keys[6], (2, F, F), F ** -0.5, 0.5),
        "input_weight": bell_draw(keys[7], (2, F, F), F ** -0.5, 0.5),
        "filter_weight": bell_draw(keys[8], (2, RBF, F), RBF ** -0.5, 0.5),
        "middle_weight": bell_draw(keys[9], (2, F, F), F ** -0.5, 0.5),
        "output_weight": bell_draw(keys[10], (2, F, F), F ** -0.5, 0.5),
    }


full_turn = 6.283185307179586

def shift_list():
    return [(along_x, along_y, along_z) for along_x in (-1, 0, 1) for along_y in (-1, 0, 1) for along_z in (-1, 0, 1)]

def wave_table(wave_index, cells_x, cells_y, cells_z):
    waves = wave_index.astype(jnp.float32)
    return (waves[0] * (full_turn / cells_x), waves[1] * (full_turn / cells_y), waves[2] * (full_turn / cells_z))

def damping_table(waves, screen_row):
    square = waves[0] * waves[0] + waves[1] * waves[1] + waves[2] * waves[2]
    damping = jnp.exp(-square[:, None] / (4.0 * screen_row[None, :]))
    return jnp.concatenate([damping, damping], axis=0)

def phase_table(coords, waves, live_flat):
    angle = coords[0][:, None] * waves[0][None, :] + coords[1][:, None] * waves[1][None, :] + coords[2][:, None] * waves[2][None, :]
    return (jnp.concatenate([jnp.cos(angle), jnp.sin(angle)], axis=1) * live_flat[:, None]).astype(jnp.bfloat16)

def cell_message(target, source, values, filter_block):
    slots = target.shape[1]
    basis_count = filter_block.shape[0]
    channels = filter_block.shape[1]
    diff = source[:3, None, :] - target[:3, :, None]
    dist = jnp.sqrt(lax.optimization_barrier(jnp.sum(diff * diff, axis=0)))
    rows = lax.broadcasted_iota(jnp.int32, dist.shape, 0)
    cols = lax.broadcasted_iota(jnp.int32, dist.shape, 1)
    keep = (cols != rows + 13 * slots).astype(jnp.float32) * source[3][None, :]
    smooth = jnp.where(dist < 1.0, 0.5 * (jnp.cos(jnp.pi * dist) + 1.0), 0.0) * keep
    centers = lax.broadcasted_iota(jnp.float32, (basis_count,), 0) / (basis_count - 1)
    gamma = 0.25 * (basis_count - 1) ** 2
    basis = jnp.exp(-gamma * (dist[:, :, None] - centers) ** 2).astype(jnp.bfloat16)
    filt = jnp.dot(basis.reshape(-1, basis_count), filter_block, preferred_element_type=jnp.float32)
    filt = (filt.reshape(slots, -1, channels) * smooth[:, :, None]).astype(jnp.bfloat16)
    return jnp.einsum('ijf,jf->if', filt.astype(jnp.float32), values.astype(jnp.float32))

def reference(features, offsets, counts, wave_index, screening, charge_weight, ewald_weight, input_weight, filter_weight, middle_weight, output_weight):
    channels = features.shape[3]
    live = (lax.broadcasted_iota(jnp.int32, (CELLS_X, CELLS_Y, GZ, A), 3) < counts[..., None]).astype(jnp.float32)
    live = live.reshape(CELLS_X, CELLS_Y, 1, GZ * A)
    geometry = jnp.concatenate([offsets, live], axis=2)
    grid_x = lax.broadcasted_iota(jnp.float32, (CELLS_X, CELLS_Y, GZ * A), 0)
    grid_y = lax.broadcasted_iota(jnp.float32, (CELLS_X, CELLS_Y, GZ * A), 1)
    grid_z = (lax.broadcasted_iota(jnp.int32, (CELLS_X, CELLS_Y, GZ * A), 2) // A).astype(jnp.float32)
    coords = jnp.stack([grid_x + offsets[:, :, 0], grid_y + offsets[:, :, 1], grid_z + offsets[:, :, 2]]).reshape(3, -1)
    waves = wave_table(wave_index, CELLS_X, CELLS_Y, GZ)
    phases = phase_table(coords, waves, live.reshape(-1))
    cells = geometry.reshape(CELLS_X, CELLS_Y, 4, GZ, A)
    pieces = []
    for along_x, along_y, along_z in shift_list():
        moved = jnp.roll(cells, (-along_x, -along_y, -along_z), axis=(0, 1, 3))
        delta = jnp.array([along_x, along_y, along_z, 0], jnp.float32)
        pieces.append(moved + delta[None, None, :, None, None])
    source_geo = jnp.stack(pieces, axis=4).transpose(0, 1, 3, 2, 4, 5).reshape(-1, 4, 27 * A)
    target_geo = cells.transpose(0, 1, 3, 2, 4).reshape(-1, 4, A)
    total = CELLS_X * CELLS_Y * GZ * A
    count_waves = wave_index.shape[1]
    state = features.reshape(-1, channels)
    for block in range(2):
        charge = jnp.dot(state, charge_weight[block], preferred_element_type=jnp.float32).astype(jnp.bfloat16)
        factors = lax.dot_general(phases, charge, (((0,), (0,)), ((), ())), preferred_element_type=jnp.float32)
        damped = (factors * damping_table(waves, screening[block]) * (2.0 / math.sqrt(total))).astype(jnp.bfloat16)
        field = jnp.dot(phases, damped, preferred_element_type=jnp.float32)
        field = (field * (1.0 / math.sqrt(count_waves))).astype(jnp.bfloat16)
        ewald_update = jax.nn.silu(jnp.dot(field, ewald_weight[block], preferred_element_type=jnp.float32))
        mapped = jnp.dot(state, input_weight[block], preferred_element_type=jnp.float32).astype(jnp.bfloat16)
        mapped = mapped.reshape(CELLS_X, CELLS_Y, GZ, A, channels)
        moved_values = [jnp.roll(mapped, (-along_x, -along_y, -along_z), axis=(0, 1, 2)) for along_x, along_y, along_z in shift_list()]
        values = jnp.stack(moved_values, axis=3).reshape(-1, 27 * A, channels)
        filter_block = filter_weight[block]

        def one_cell(item):
            return cell_message(item[0], item[1], item[2], filter_block)
        messages = lax.map(one_cell, (target_geo, source_geo, values))
        messages = messages.reshape(-1, channels).astype(jnp.bfloat16)
        middle = jax.nn.silu(jnp.dot(messages, middle_weight[block], preferred_element_type=jnp.float32)).astype(jnp.bfloat16)
        conv_update = jnp.dot(middle, output_weight[block], preferred_element_type=jnp.float32)
        state = (state.astype(jnp.float32) + ewald_update + conv_update).astype(jnp.bfloat16)
    return state.reshape(features.shape)
```

```python
import functools
import math

import jax
import jax.numpy as jnp
from jax import lax
from jax.experimental import pallas as pl
from jax.experimental.pallas import tpu as pltpu
from jax.sharding import PartitionSpec as P


f32 = jnp.float32
bf16 = jnp.bfloat16

LANES = 128
PARTS = 3
GEO = 16
LIVE = 9
CHUNK = 256
GROUP = 16
NONE = -1.0e30

COS_TURN = (
    1.0,
    -19.73920440673828,
    64.93911743164062,
    -85.45011138916016,
    60.16743087768555,
    -25.96688461303711,
    6.527706146240234,
)
SIN_TURN = (
    6.2831854820251465,
    -41.34170150756836,
    81.60513305664062,
    -76.7030029296875,
    42.02585220336914,
    -14.899578094482422,
    3.2377800941467285,
)
COS_HALF = (
    1.0,
    -1.2337005138397217,
    0.2536693215370178,
    -0.02086268737912178,
    0.000917722936719656,
    -2.3824151867302135e-05,
)


def power_sum(terms, x):
    out = terms[-1] * x + terms[-2]
    for term in terms[-3::-1]:
        out = out * x + term
    return out


def mm(a, b):
    return jnp.dot(a, b, preferred_element_type=f32)


def mm_nt(a, b):
    return lax.dot_general(a, b, (((1,), (1,)), ((), ())), preferred_element_type=f32)


def mm_tn(a, b):
    return lax.dot_general(a, b, (((0,), (0,)), ((), ())), preferred_element_type=f32)


def silu(t):
    return t / (1.0 + jnp.exp(-t))


def iota(shape, dim):
    return lax.broadcasted_iota(jnp.int32, shape, dim)


def vmem():
    return pl.BlockSpec(memory_space=pltpu.VMEM)


def smem():
    return pl.BlockSpec(memory_space=pltpu.SMEM)


def pack_kernel(depth, slots, counts_ref, features_ref, offsets_ref, out_ref):
    atoms, channels = features_ref.shape
    out_ref[0:atoms, :] = features_ref[...]
    rows = []
    for axis in range(3):
        rest = offsets_ref[axis : axis + 1, :]
        for _ in range(PARTS):
            piece = rest.astype(bf16).astype(f32)
            rows.append(piece)
            rest = rest - piece
    lane = iota((1, atoms), 1)
    limit = jnp.zeros((1, atoms), jnp.int32)
    for cell in range(depth):
        limit = jnp.where(lane // slots == cell, counts_ref[cell], limit)
    rows.append((lane - (lane // slots) * slots < limit).astype(f32))
    rows.append(jnp.zeros((GEO - len(rows), atoms), f32))
    out_ref[atoms : atoms + GEO, :] = jnp.concatenate(rows, axis=0).astype(bf16)


def places(live):
    rows, atoms = live.shape
    before = (iota((atoms, atoms), 0) < iota((atoms, atoms), 1)).astype(f32).astype(bf16)
    ones = jnp.ones((atoms, atoms), bf16)
    live_b = live.astype(bf16)
    inside = mm(live_b, before)
    total = mm(live_b, ones)
    above = (iota((rows, rows), 1) < iota((rows, rows), 0)).astype(f32).astype(bf16)
    start = mm(above, total.astype(bf16))
    place = jnp.where(live > 0.0, inside + start, -1.0)
    return place, jnp.sum(live).astype(jnp.int32)


def chosen(place, columns, first, size):
    atoms = place.shape[1]
    want = (iota((size, atoms), 0) + first).astype(f32)
    return [
        jnp.where(want == place[c : c + 1, :], 1.0, 0.0).astype(bf16) for c in range(columns)
    ]


def joined(rows):
    return (rows[0] + rows[1]) + rows[2]


def conv_kernel(
    depth,
    slots,
    near,
    target_ref,
    geo_a,
    geo_b,
    geo_c,
    state_a,
    state_b,
    state_c,
    own_ref,
    input_ref,
    filter_ref,
    middle_ref,
    output_ref,
    out_ref,
    mapped_ref,
    place_ref,
    scale_ref,
    weight_ref,
    basis_ref,
    sums_ref,
    center_ref,
    message_ref,
):
    atoms, channels = own_ref.shape
    count = filter_ref.shape[0]
    spread = math.sqrt(0.25 * math.log2(math.e))
    geo = (geo_a, geo_b, geo_c)
    state = (state_a, state_b, state_c)
    columns = len(near)
    lives = []
    for c, (plane, row, _, _) in enumerate(near):
        mapped_ref[c * atoms : (c + 1) * atoms, :] = mm(
            state[plane][row, 0:atoms, :], input_ref[...]
        ).astype(bf16)
        lives.append(geo[plane][row, atoms + LIVE : atoms + LIVE + 1, :].astype(f32))
    pad = -columns % 8
    live = jnp.concatenate(lives + [jnp.zeros((pad, atoms), f32)], axis=0)
    place, total = places(live)
    place_ref[...] = place
    center_ref[...] = iota((count, LANES), 0).astype(f32) * spread
    message_ref[...] = jnp.zeros_like(message_ref)
    own = target_ref[...]
    own_x, own_y, own_z = own[:, 0:1], own[:, 1:2], own[:, 2:3]
    lane = iota((1, atoms), 1)

    def chunk_step(chunk, carry):
        first = chunk * CHUNK
        rows = chosen(place_ref[...], columns, first, CHUNK)
        mapped = mm(jnp.concatenate(rows, axis=1), mapped_ref[...]).astype(bf16)
        found = jnp.zeros((2 * GEO, CHUNK), f32)
        for c, (plane, row, along_x, along_y) in enumerate(near):
            home = along_x == 0 and along_y == 0
            extra = jnp.concatenate(
                [
                    jnp.full((1, atoms), along_x, f32),
                    jnp.full((1, atoms), along_y, f32),
                    (lane // slots).astype(f32),
                    (lane + 1).astype(f32) if home else jnp.zeros((1, atoms), f32),
                    jnp.zeros((GEO - 4, atoms), f32),
                ],
                axis=0,
            ).astype(bf16)
            known = jnp.concatenate([geo[plane][row, atoms : atoms + GEO, :], extra], axis=0)
            found = found + mm_nt(known, rows[c])
        at = [joined([found[PARTS * a + p : PARTS * a + p + 1] for p in range(PARTS)]) for a in range(3)]
        along = [found[GEO + a : GEO + a + 1] for a in range(4)]
        who = iota((atoms, CHUNK), 0)
        layer = (who // slots).astype(f32)
        step_z = along[2] - layer
        step_z = jnp.where(step_z > 0.5 * depth, step_z - depth, step_z)
        step_z = jnp.where(step_z < -0.5 * depth, step_z + depth, step_z)
        diff_x = (along[0] + at[0]) - own_x
        diff_y = (along[1] + at[1]) - own_y
        diff_z = (step_z + at[2]) - own_z
        square = diff_x * diff_x + diff_y * diff_y + diff_z * diff_z
        dist = jnp.sqrt(square)
        kept = jnp.logical_and(dist < 1.0, along[3] != (who + 1).astype(f32))
        kept = jnp.logical_and(kept, iota((atoms, CHUNK), 1) + first < total)
        half = jnp.maximum(power_sum(COS_HALF, jnp.minimum(square, 1.0)), 1.0e-18)
        weight_ref[...] = jnp.where(kept, 2.0 * jnp.log2(half), NONE)
        scale_ref[...] = dist * ((count - 1) * spread)

        def group_step(g, carry):
            start = pl.multiple_of(g * GROUP, GROUP)
            scale = scale_ref[pl.ds(start, GROUP), :]
            weight = weight_ref[pl.ds(start, GROUP), :]
            for i in range(GROUP):
                for half_lane in range(CHUNK // LANES):
                    part = slice(half_lane * LANES, (half_lane + 1) * LANES)
                    away = scale[i : i + 1, part] - center_ref[...]
                    basis_ref[i * count : (i + 1) * count, part] = jnp.exp2(
                        weight[i : i + 1, part] - away * away
                    ).astype(bf16)
            sums_ref[...] = mm(basis_ref[...], mapped)
            filt = filter_ref[...].astype(f32)
            lines = []
            for i in range(GROUP):
                mixed = sums_ref[i * count : (i + 1) * count, :] * filt
                lines.append(jnp.sum(mixed, axis=0, keepdims=True))
            message_ref[pl.ds(start, GROUP), :] += jnp.concatenate(lines, axis=0)
            return carry

        lax.fori_loop(0, atoms // GROUP, group_step, 0)
        return carry

    lax.fori_loop(0, (total + CHUNK - 1) // CHUNK, chunk_step, 0)
    middle = silu(mm(message_ref[...].astype(bf16), middle_ref[...])).astype(bf16)
    out_ref[...] = mm(middle, output_ref[...])


def turns(wave, x, y, z):
    angle = wave[0] * x + wave[1] * y + wave[2] * z
    return angle - jnp.round(angle)


def phase_rows(wave_ref, x, y, z, out_ref):
    waves = wave_ref.shape[1]
    lanes = x.shape[1]
    for first in range(0, waves, 64):
        part = slice(first, first + 64)
        rest = turns([wave_ref[a, part, :] for a in range(3)], x, y, z)
        square = rest * rest
        out_ref[part, :] = power_sum(COS_TURN, square).astype(bf16)
        out_ref[waves + first : waves + first + 64, :] = (
            power_sum(SIN_TURN, square) * rest
        ).astype(bf16)


def ewald_kernel(
    depth,
    slots,
    total_atoms,
    place_of_ref,
    wave_ref,
    screen_ref,
    geo_ref,
    state_ref,
    own_ref,
    conv_ref,
    charge_ref,
    update_ref,
    out_ref,
    table_ref,
    own_phase_ref,
    phase_ref,
    factor_ref,
    damp_ref,
):
    planes, columns = geo_ref.shape[0], geo_ref.shape[1]
    atoms, channels = own_ref.shape
    waves = wave_ref.shape[0]
    ring_x, ring_y = place_of_ref[2], place_of_ref[3]
    here_x, here_y = place_of_ref[0], place_of_ref[1]
    inv_x = 1.0 / planes
    inv_y = 1.0 / columns
    inv_z = 1.0 / depth
    wave = wave_ref[...].astype(f32)
    for a in range(3):
        table_ref[a, :, :] = jnp.broadcast_to(wave[:, a : a + 1], (waves, LANES))
    lane = iota((1, atoms), 1)
    layer = (lane // slots).astype(f32)

    def column_at(known, x0, y0):
        spot = [joined([known[PARTS * a + p : PARTS * a + p + 1] for p in range(PARTS)]) for a in range(3)]
        return (x0 + spot[0]) * inv_x, (y0 + spot[1]) * inv_y, spot[2]

    factor_ref[...] = jnp.zeros_like(factor_ref)

    def plane_step(s, carry):
        x0 = lax.rem(here_x - s + planes, planes).astype(f32)
        lives = [geo_ref[s, t, atoms + LIVE : atoms + LIVE + 1, :].astype(f32) for t in range(columns)]
        pad = -columns % 8
        live = jnp.concatenate(lives + [jnp.zeros((pad, atoms), f32)] * (pad > 0), axis=0)
        place, total = places(live)

        def tile_step(j, carry):
            rows = chosen(place, columns, j * LANES, LANES)
            picked = jnp.zeros((LANES, channels), f32)
            known = jnp.zeros((2 * GEO, LANES), f32)
            for t in range(columns):
                picked = picked + mm(rows[t], state_ref[s, t, 0:atoms, :])
                y0 = lax.rem(here_y - t + columns, columns).astype(f32)
                extra = jnp.concatenate(
                    [jnp.zeros((1, atoms), f32) + y0, layer, jnp.zeros((GEO - 2, atoms), f32)], axis=0
                ).astype(bf16)
                full = jnp.concatenate([geo_ref[s, t, atoms : atoms + GEO, :], extra], axis=0)
                known = known + mm_nt(full, rows[t])
            charge = mm(picked.astype(bf16), charge_ref[...]).astype(bf16)
            x, y, z = column_at(known, x0, known[GEO : GEO + 1])
            z = (known[GEO + 1 : GEO + 2] + z) * inv_z
            phase_rows(table_ref, x, y, z, phase_ref)
            factor_ref[...] += mm(phase_ref[...], charge)
            return carry

        return lax.fori_loop(0, (total + LANES - 1) // LANES, tile_step, carry)

    lax.fori_loop(0, planes, plane_step, 0)

    own_geo = geo_ref[0, 0, atoms : atoms + GEO, :].astype(f32)
    x, y, z = column_at(own_geo, here_x.astype(f32), here_y.astype(f32))
    z = (layer + z) * inv_z
    phase_rows(table_ref, x, y, z, own_phase_ref)
    own_live = own_geo[LIVE : LIVE + 1].astype(bf16)

    full_turn = 6.283185307179586
    kx = table_ref[0] * (full_turn / planes)
    ky = table_ref[1] * (full_turn / columns)
    kz = table_ref[2] * (full_turn / depth)
    damp_ref[...] = jnp.exp(-(kx * kx + ky * ky + kz * kz) / (4.0 * screen_ref[...]))
    norm = 2.0 / math.sqrt(total_atoms)
    for side in range(2):
        part = slice(side * waves, (side + 1) * waves)
        factor_ref[part, :] = factor_ref[part, :] * damp_ref[...] * norm
    damped = factor_ref[...].astype(bf16)
    field = mm_tn(own_phase_ref[...] * own_live, damped)
    field = (field * (1.0 / math.sqrt(waves))).astype(bf16)
    ewald = silu(mm(field, update_ref[...]))
    out_ref[...] = (own_ref[...].astype(f32) + ewald + conv_ref[...]).astype(bf16)


def gathered(rows, axis):
    size = lax.axis_size(axis)
    moved = [rows]
    near = [1, size - 1]
    for shift in near + list(range(2, size - 1)):
        moved.append(lax.ppermute(rows, axis, [(i, (i + shift) % size) for i in range(size)]))
    order = [0] + near + list(range(2, size - 1))
    return [moved[order.index(i)] for i in range(size)]


def shards(
    features,
    offsets,
    counts,
    wave_index,
    screening,
    charge_weight,
    ewald_weight,
    input_weight,
    filter_weight,
    middle_weight,
    output_weight,
):
    depth = counts.shape[2]
    atoms, channels = features.shape[2:]
    slots = atoms // depth
    nx = lax.axis_size("gx")
    ny = lax.axis_size("gy")
    waves = wave_index.shape[1]
    assert atoms == LANES and channels == LANES and waves % 64 == 0
    state = features.reshape(atoms, channels)
    spots = offsets.reshape(3, atoms)
    payload = pl.pallas_call(
        functools.partial(pack_kernel, depth, slots),
        out_shape=jax.ShapeDtypeStruct((atoms + GEO, channels), bf16),
        in_specs=[smem(), vmem(), vmem()],
        out_specs=vmem(),
        name="pack",
    )(counts.reshape(depth), state, spots)
    target = jnp.pad(spots.T, ((0, 0), (0, 5)))
    wave_rows = jnp.pad(wave_index.T, ((0, 0), (0, 5)))
    here = jnp.stack([lax.axis_index("gx"), lax.axis_index("gy"), jnp.int32(nx), jnp.int32(ny)])

    near = []
    for plane, s, along_x in ((0, 0, 0), (1, 1, -1), (2, nx - 1, 1)):
        for t, along_y in ((0, 0), (1, -1), (ny - 1, 1)):
            near.append((plane, t, along_x, along_y))

    def spread_out(rows):
        return gathered(jnp.stack(gathered(rows, "gy")), "gx")

    conv_call = pl.pallas_call(
        functools.partial(conv_kernel, depth, slots, tuple(near)),
        out_shape=jax.ShapeDtypeStruct((atoms, channels), f32),
        in_specs=[vmem() for _ in range(12)],
        out_specs=vmem(),
        scratch_shapes=[
            pltpu.VMEM((len(near) * atoms, channels), bf16),
            pltpu.VMEM((len(near) + -len(near) % 8, atoms), f32),
            pltpu.VMEM((atoms, CHUNK), f32),
            pltpu.VMEM((atoms, CHUNK), f32),
            pltpu.VMEM((GROUP * filter_weight.shape[1], CHUNK), bf16),
            pltpu.VMEM((GROUP * filter_weight.shape[1], channels), f32),
            pltpu.VMEM((filter_weight.shape[1], LANES), f32),
            pltpu.VMEM((atoms, channels), f32),
        ],
        name="conv",
    )
    ewald_call = pl.pallas_call(
        functools.partial(ewald_kernel, depth, slots, nx * ny * atoms),
        out_shape=jax.ShapeDtypeStruct((atoms, channels), bf16),
        in_specs=[smem()] + [vmem() for _ in range(8)],
        out_specs=vmem(),
        scratch_shapes=[
            pltpu.VMEM((3, waves, LANES), f32),
            pltpu.VMEM((2 * waves, LANES), bf16),
            pltpu.VMEM((2 * waves, LANES), bf16),
            pltpu.VMEM((2 * waves, channels), f32),
            pltpu.VMEM((waves, channels), f32),
        ],
        name="ewald",
    )
    geo_planes = spread_out(payload)
    geo_all = jnp.stack(geo_planes)
    state_planes, state_all = geo_planes, geo_all
    for block in range(2):
        if block:
            state_planes = spread_out(state)
            state_all = jnp.stack(state_planes)
        conv = conv_call(
            target,
            geo_planes[0],
            geo_planes[1],
            geo_planes[nx - 1],
            state_planes[0],
            state_planes[1],
            state_planes[nx - 1],
            state,
            input_weight[block],
            filter_weight[block],
            middle_weight[block],
            output_weight[block],
        )
        state = ewald_call(
            here,
            wave_rows,
            screening[block : block + 1],
            geo_all,
            state_all,
            state,
            conv,
            charge_weight[block],
            ewald_weight[block],
        )
    return state.reshape(features.shape)


def solution(mesh):
    in_specs = (
        P("gx", "gy", None, None),
        P("gx", "gy", None, None),
        P("gx", "gy", None),
        P(),
        P(),
        P(),
        P(),
        P(),
        P(),
        P(),
        P(),
    )
    out_specs = P("gx", "gy", None, None)
    return jax.shard_map(shards, mesh=mesh, in_specs=in_specs, out_specs=out_specs, check_vma=False)
```

```python
import functools
import math

import jax
import jax.numpy as jnp
from jax import lax
from jax.experimental import pallas as pl
from jax.experimental.pallas import tpu as pltpu
from jax.sharding import PartitionSpec as P


f32 = jnp.float32
bf16 = jnp.bfloat16

LANES = 128
PARTS = 3
GEO = 16
LIVE, SPOT_X, SPOT_Y, LAYER, SLOT = 9, 10, 11, 12, 13
CHUNK = 256
GROUP = 16
NONE = -1.0e30

COS_TURN = (
    1.0,
    -19.73920440673828,
    64.93911743164062,
    -85.45011138916016,
    60.16743087768555,
    -25.96688461303711,
    6.527706146240234,
)
SIN_TURN = (
    6.2831854820251465,
    -41.34170150756836,
    81.60513305664062,
    -76.7030029296875,
    42.02585220336914,
    -14.899578094482422,
    3.2377800941467285,
)
COS_HALF = (
    1.0,
    -1.2337005138397217,
    0.2536693215370178,
    -0.02086268737912178,
    0.000917722936719656,
    -2.3824151867302135e-05,
)


def power_sum(terms, x):
    out = terms[-1] * x + terms[-2]
    for term in terms[-3::-1]:
        out = out * x + term
    return out


def mm(a, b):
    return jnp.dot(a, b, preferred_element_type=f32)


def mm_nt(a, b):
    return lax.dot_general(a, b, (((1,), (1,)), ((), ())), preferred_element_type=f32)


def mm_tn(a, b):
    return lax.dot_general(a, b, (((0,), (0,)), ((), ())), preferred_element_type=f32)


def silu(t):
    return t / (1.0 + jnp.exp(-t))


def iota(shape, dim):
    return lax.broadcasted_iota(jnp.int32, shape, dim)


def vmem():
    return pl.BlockSpec(memory_space=pltpu.VMEM)


def smem():
    return pl.BlockSpec(memory_space=pltpu.SMEM)


def pack_kernel(counts_ref, features_ref, offsets_ref, out_ref):
    depth = counts_ref.shape[2]
    atoms, _ = features_ref.shape[2:]
    slots = atoms // depth
    out_ref[0:atoms, :] = features_ref[0, 0]
    rows = []
    for axis in range(3):
        rest = offsets_ref[0, 0, axis : axis + 1, :]
        for _ in range(PARTS):
            piece = rest.astype(bf16).astype(f32)
            rows.append(piece)
            rest = rest - piece
    lane = iota((1, atoms), 1)
    limit = jnp.zeros((1, atoms), jnp.int32)
    for cell in range(depth):
        limit = jnp.where(lane // slots == cell, counts_ref[0, 0, cell], limit)
    rows.append((lane - (lane // slots) * slots < limit).astype(f32))
    rows.append(jnp.full((1, atoms), lax.axis_index("gx"), jnp.int32).astype(f32))
    rows.append(jnp.full((1, atoms), lax.axis_index("gy"), jnp.int32).astype(f32))
    rows.append((lane // slots).astype(f32))
    rows.append((lane + 1).astype(f32))
    rows.append(jnp.zeros((GEO - len(rows), atoms), f32))
    out_ref[atoms : atoms + GEO, :] = jnp.concatenate(rows, axis=0).astype(bf16)


def places(live, span):
    rows, atoms = live.shape
    before = (iota((atoms, atoms), 0) < iota((atoms, atoms), 1)).astype(f32).astype(bf16)
    live_b = live.astype(bf16)
    inside = mm(live_b, before)
    total = mm(live_b, jnp.ones((atoms, atoms), bf16))
    row, other = iota((rows, rows), 0), iota((rows, rows), 1)
    above = jnp.logical_and(other < row, other // span == row // span).astype(f32).astype(bf16)
    return jnp.where(live > 0.0, inside + mm(above, total.astype(bf16)), -1.0)


def chosen(place, first, size):
    want = (iota((size, place.shape[1]), 0) + first).astype(f32)
    return jnp.concatenate(
        [jnp.where(want == place[c : c + 1, :], 1.0, 0.0).astype(bf16) for c in range(place.shape[0])],
        axis=1,
    )


def identity(rows, columns):
    return (iota((rows, columns), 0) == iota((rows, columns), 1)).astype(f32).astype(bf16)


def joined(known, axis):
    parts = [known[PARTS * axis + p : PARTS * axis + p + 1] for p in range(PARTS)]
    return (parts[0] + parts[1]) + parts[2]


def grouped(known, groups):
    out = known[0:GEO]
    for g in range(1, groups):
        out = out + known[g * GEO : (g + 1) * GEO]
    return out


def wrapped(step, size):
    step = jnp.where(step > 0.5 * size, step - size, step)
    return jnp.where(step < -0.5 * size, step + size, step)


def outside(x):
    return jnp.maximum(jnp.maximum(-x, x - 1.0), 0.0)


def conv_kernel(
    depth,
    slots,
    size_x,
    size_y,
    rows_of,
    index,
    geo_a,
    geo_b,
    geo_c,
    state_a,
    state_b,
    state_c,
    input_ref,
    filter_ref,
    middle_ref,
    output_ref,
    out_ref,
    source_ref,
    place_ref,
    scale_ref,
    weight_ref,
    basis_ref,
    wide_ref,
    center_ref,
    message_ref,
    mapped_ref,
):
    atoms, channels = message_ref.shape
    count = filter_ref.shape[1]
    spread = math.sqrt(0.25 * math.log2(math.e))
    geo = (geo_a, geo_b, geo_c)
    state = (state_a, state_b, state_c)
    near = len(rows_of)
    columns = 3 * near
    block = columns + -columns % 8
    eye = identity(atoms, atoms)
    spots = [[], [], [], [], [], []]
    for plane in range(3):
        known = jnp.concatenate([geo[plane][row, atoms : atoms + GEO, :] for row in rows_of], axis=0)
        turned = mm_nt(eye, known)
        group = iota(turned.shape, 1) // GEO
        wide = known.astype(f32)
        if plane == 0:
            here_x = wide[SPOT_X : SPOT_X + 1, 0:1]
            here_y = wide[SPOT_Y : SPOT_Y + 1, 0:1]
            target = [
                (turned[:, PARTS * a : PARTS * a + 1] + turned[:, PARTS * a + 1 : PARTS * a + 2])
                + turned[:, PARTS * a + 2 : PARTS * a + 3]
                for a in range(3)
            ]
        for i, row in enumerate(rows_of):
            part = slice((plane * near + i) * atoms, (plane * near + i + 1) * atoms)
            source_ref[part, 0:channels] = mm(state[plane][row, 0:atoms, :], input_ref[index]).astype(bf16)
            source_ref[part, channels : channels + near * GEO] = jnp.where(group == i, turned, 0.0).astype(bf16)
            own = wide[i * GEO : (i + 1) * GEO]
            for a in range(3):
                spots[a].append(joined(own, a))
            for a, r in ((3, LIVE), (4, SPOT_X), (5, SPOT_Y)):
                spots[a].append(own[r : r + 1])
    fill = [jnp.zeros((block - columns, atoms), f32)]
    x, y, z, live, at_x, at_y = [jnp.concatenate(rows + fill, axis=0) for rows in spots]
    out_x = outside(wrapped(at_x - here_x, size_x) + x)
    out_y = outside(wrapped(at_y - here_y, size_y) + y)
    flat = out_x * out_x + out_y * out_y
    layers = (iota((block, atoms), 1) // slots).astype(f32)
    lives = []
    longest = jnp.int32(0)
    totals = []
    for cell in range(depth):
        out_z = outside(wrapped(layers - float(cell), depth) + z)
        close = jnp.where(flat + out_z * out_z < 1.001, live, 0.0)
        lives.append(close)
        totals.append(jnp.sum(close).astype(jnp.int32))
        longest = jnp.maximum(longest, totals[-1])
    place_ref[...] = places(jnp.concatenate(lives, axis=0), block)
    center_ref[...] = iota((count, CHUNK), 0).astype(f32) * spread
    wide_ref[...] = filter_ref[index].astype(f32)
    message_ref[...] = jnp.zeros_like(message_ref)
    pick_rows = identity(near * GEO, atoms)

    def piece(first, width):
        for cell in range(depth):
            want = chosen(place_ref[cell * block : cell * block + columns, :], first, width)
            found = mm(want, source_ref[...])
            mapped_ref[cell, 0:width, :] = found[:, 0:channels].astype(bf16)
            known = grouped(mm_nt(pick_rows, found[:, channels : 2 * channels].astype(bf16)), near)
            part = slice(cell * slots, (cell + 1) * slots)
            along_x = wrapped(known[SPOT_X : SPOT_X + 1] - here_x, size_x)
            along_y = wrapped(known[SPOT_Y : SPOT_Y + 1] - here_y, size_y)
            along_z = wrapped(known[LAYER : LAYER + 1] - float(cell), depth)
            home = jnp.abs(along_x) + jnp.abs(along_y)
            who = jnp.where(home == 0.0, known[SLOT : SLOT + 1], 0.0)
            diff_x = (along_x + joined(known, 0)) - target[0][part, :]
            diff_y = (along_y + joined(known, 1)) - target[1][part, :]
            diff_z = (along_z + joined(known, 2)) - target[2][part, :]
            square = diff_x * diff_x + diff_y * diff_y + diff_z * diff_z
            dist = jnp.sqrt(square)
            mine = (iota((slots, width), 0) + (cell * slots + 1)).astype(f32)
            kept = jnp.logical_and(dist < 1.0, who != mine)
            kept = jnp.logical_and(kept, iota((slots, width), 1) + first < totals[cell])
            half = jnp.maximum(power_sum(COS_HALF, jnp.minimum(square, 1.0)), 1.0e-18)
            weight_ref[part, 0:width] = jnp.where(kept, 2.0 * jnp.log2(half), NONE)
            scale_ref[part, 0:width] = dist * ((count - 1) * spread)

        def group_step(g, carry):
            start = pl.multiple_of(g * GROUP, GROUP)
            scale = scale_ref[pl.ds(start, GROUP), 0:width]
            weight = weight_ref[pl.ds(start, GROUP), 0:width]
            for i in range(GROUP):
                away = scale[i : i + 1, :] - center_ref[:, 0:width]
                basis_ref[i * count : (i + 1) * count, 0:width] = jnp.exp2(
                    weight[i : i + 1, :] - away * away
                ).astype(bf16)
            sums = mm(basis_ref[:, 0:width], mapped_ref[g // (slots // GROUP), 0:width, :])
            lines = []
            for i in range(GROUP):
                mixed = sums[i * count : (i + 1) * count, :] * wide_ref[...]
                lines.append(jnp.sum(mixed, axis=0, keepdims=True))
            message_ref[pl.ds(start, GROUP), :] += jnp.concatenate(lines, axis=0)
            return carry

        lax.fori_loop(0, atoms // GROUP, group_step, 0)

    full = (longest + (LANES - 1)) // CHUNK

    def chunk_step(chunk, carry):
        piece(chunk * CHUNK, CHUNK)
        return carry

    lax.fori_loop(0, full, chunk_step, 0)

    @pl.when(full * CHUNK < longest)
    def _():
        piece(full * CHUNK, LANES)

    middle = silu(mm(message_ref[...].astype(bf16), middle_ref[index])).astype(bf16)
    out_ref[...] = mm(middle, output_ref[index])


def phase_rows(wave_ref, x, y, z, put):
    waves = wave_ref.shape[1]
    step = 64
    for first in range(0, waves, step):
        part = slice(first, first + step)
        kx, ky, kz = [
            jnp.concatenate([wave_ref[a, part, :]] * (x.shape[1] // LANES), axis=1) for a in range(3)
        ]
        angle = kx * x + ky * y + kz * z
        rest = angle - jnp.round(angle)
        square = rest * rest
        put(first, power_sum(COS_TURN, square).astype(bf16))
        put(waves + first, (power_sum(SIN_TURN, square) * rest).astype(bf16))


def ewald_first(depth, total_atoms, index, wave_ref, screen_ref, geo_ref, *refs):
    ewald_body(depth, total_atoms, index, wave_ref, screen_ref, geo_ref, geo_ref, *refs)


def ewald_body(
    depth,
    total_atoms,
    index,
    wave_ref,
    screen_ref,
    geo_ref,
    state_ref,
    own_ref,
    conv_ref,
    charge_ref,
    update_ref,
    out_ref,
    table_ref,
    own_phase_ref,
    phase_ref,
    factor_ref,
    damp_ref,
    turned_ref,
    place_ref,
    packed_state_ref,
    packed_geo_ref,
    tile_charge_ref,
    tile_spot_ref,
    first_ref,
    number_ref,
):
    planes, columns = geo_ref.shape[0], geo_ref.shape[1]
    atoms, channels = own_ref.shape
    waves = wave_ref.shape[1]
    eye = identity(atoms, atoms)
    numbers = jnp.concatenate([wave_ref[...].astype(f32), jnp.zeros((5, waves), f32)], axis=0).astype(bf16)
    for first in range(0, waves, LANES):
        turned = mm_nt(eye, numbers[:, first : first + LANES])
        for a in range(3):
            table_ref[a, first : first + LANES, :] = jnp.broadcast_to(turned[:, a : a + 1], (LANES, LANES))
    block = columns + -columns % 8

    def plane_live(s, carry):
        lives = [geo_ref[s, t, atoms + LIVE : atoms + LIVE + 1, :].astype(f32) for t in range(columns)]
        if block > columns:
            lives.append(jnp.zeros((block - columns, atoms), f32))
        live = jnp.concatenate(lives, axis=0)
        place_ref[pl.ds(pl.multiple_of(s * block, block), block), :] = live
        known = jnp.concatenate([geo_ref[s, t, atoms : atoms + GEO, :] for t in range(columns)], axis=0)
        if columns * GEO < LANES:
            known = jnp.concatenate([known, jnp.zeros((LANES - columns * GEO, atoms), bf16)], axis=0)
        turned = mm_nt(eye, known)
        group = iota(turned.shape, 1) // GEO
        for t in range(columns):
            turned_ref[s, t * atoms : (t + 1) * atoms, :] = jnp.where(group == t, turned, 0.0).astype(bf16)
        number = jnp.sum(live).astype(jnp.int32)
        number_ref[s] = number
        first_ref[s] = carry[0]
        return carry[0] + number, jnp.maximum(carry[1], number)

    unroll = 8 if planes % 8 == 0 else 1
    total, most = lax.fori_loop(0, planes, plane_live, (jnp.int32(0), jnp.int32(0)), unroll=unroll)
    place_ref[...] = places(place_ref[...], block)
    pairs = (total + (CHUNK - 1)) // CHUNK

    def clear(p, carry):
        packed_state_ref[pl.ds(pl.multiple_of(p * LANES, LANES), LANES), :] = jnp.zeros((LANES, channels), f32)
        packed_geo_ref[pl.ds(pl.multiple_of(p * LANES, LANES), LANES), :] = jnp.zeros((LANES, LANES), f32)
        return carry

    lax.fori_loop(0, 2 * pairs + 2, clear, 0)

    def pick_step(j, carry):
        def plane_step(s, carry):
            start = pl.multiple_of(s * block, block)
            place = place_ref[pl.ds(start, block), :][0:columns]
            want = chosen(place, j * LANES, LANES)
            picked = mm(want, state_ref[s, :, 0:atoms, :].reshape(columns * atoms, channels))
            spots = mm(want, turned_ref[s])

            @pl.when(j * LANES < number_ref[s])
            def _():
                rows = pl.ds(first_ref[s] + j * LANES, LANES)
                packed_state_ref[rows, :] += picked
                packed_geo_ref[rows, :] += spots

            return carry

        return lax.fori_loop(0, planes, plane_step, carry, unroll=unroll)

    lax.fori_loop(0, (most + (LANES - 1)) // LANES, pick_step, 0)

    def places_of(known):
        x = (known[SPOT_X : SPOT_X + 1] + joined(known, 0)) * (1.0 / planes)
        y = (known[SPOT_Y : SPOT_Y + 1] + joined(known, 1)) * (1.0 / columns)
        z = (known[LAYER : LAYER + 1] + joined(known, 2)) * (1.0 / depth)
        return x, y, z

    def prepare(p):
        rows = pl.ds(pl.multiple_of(p * CHUNK, CHUNK), CHUNK)
        slot = lax.rem(p, 2)
        tile_charge_ref[slot] = mm(packed_state_ref[rows, :].astype(bf16), charge_ref[index]).astype(bf16)
        known = grouped(mm_nt(eye, packed_geo_ref[rows, :].astype(bf16)), columns)
        tile_spot_ref[slot, 0:3, :] = jnp.concatenate(places_of(known), axis=0)

    own_geo = geo_ref[0, 0, atoms : atoms + GEO, :].astype(f32)
    x, y, z = places_of(own_geo)

    def put_own(first, value):
        own_phase_ref[first : first + value.shape[0], :] = value

    phase_rows(table_ref, x, y, z, put_own)
    own_live = own_geo[LIVE : LIVE + 1].astype(bf16)
    factor_ref[...] = jnp.zeros_like(factor_ref)
    prepare(jnp.int32(0))

    def pair_step(p, carry):
        slot = lax.rem(p, 2)
        spot = tile_spot_ref[slot]
        charge = tile_charge_ref[slot]

        def put(first, value):
            phase_ref[first : first + value.shape[0], :] = value

        phase_rows(table_ref, spot[0:1], spot[1:2], spot[2:3], put)
        factor_ref[...] += mm(phase_ref[...], charge)
        prepare(jnp.minimum(p + 1, pairs - 1))
        return carry

    lax.fori_loop(0, pairs, pair_step, 0)

    full_turn = 6.283185307179586
    kx = table_ref[0] * (full_turn / planes)
    ky = table_ref[1] * (full_turn / columns)
    kz = table_ref[2] * (full_turn / depth)
    damp_ref[...] = jnp.exp(-(kx * kx + ky * ky + kz * kz) / (4.0 * screen_ref[index : index + 1, :]))
    norm = 2.0 / math.sqrt(total_atoms)
    for side in range(2):
        part = slice(side * waves, (side + 1) * waves)
        factor_ref[part, :] = factor_ref[part, :] * damp_ref[...] * norm
    damped = factor_ref[...].astype(bf16)
    field = mm_tn(own_phase_ref[...] * own_live, damped)
    field = (field * (1.0 / math.sqrt(waves))).astype(bf16)
    ewald = silu(mm(field, update_ref[index]))
    out_ref[...] = (own_ref[...].astype(f32) + ewald + conv_ref[...]).astype(bf16)


def gathered(rows, axis):
    size = lax.axis_size(axis)
    moved = [rows]
    near = [1, size - 1]
    for shift in near + list(range(2, size - 1)):
        moved.append(lax.ppermute(rows, axis, [(i, (i + shift) % size) for i in range(size)]))
    order = [0] + near + list(range(2, size - 1))
    return [moved[order.index(i)] for i in range(size)]


def shards(
    features,
    offsets,
    counts,
    wave_index,
    screening,
    charge_weight,
    ewald_weight,
    input_weight,
    filter_weight,
    middle_weight,
    output_weight,
):
    depth = counts.shape[2]
    atoms, channels = features.shape[2:]
    slots = atoms // depth
    nx = lax.axis_size("gx")
    ny = lax.axis_size("gy")
    waves = wave_index.shape[1]
    assert atoms == LANES and channels == LANES and waves % 64 == 0
    state = features.reshape(atoms, channels)
    payload = pl.pallas_call(
        pack_kernel,
        out_shape=jax.ShapeDtypeStruct((atoms + GEO, channels), bf16),
        in_specs=[smem(), vmem(), vmem()],
        out_specs=vmem(),
        name="pack",
    )(counts, features, offsets)

    rows_of = (0, 1, ny - 1)
    columns = 3 * len(rows_of)
    tall = columns + -columns % 8
    count = filter_weight.shape[1]

    def spread_out(rows):
        return gathered(jnp.stack(gathered(rows, "gy")), "gx")

    conv_call = lambda index: pl.pallas_call(
        functools.partial(conv_kernel, depth, slots, nx, ny, rows_of, index),
        out_shape=jax.ShapeDtypeStruct((atoms, channels), f32),
        in_specs=[vmem() for _ in range(10)],
        out_specs=vmem(),
        scratch_shapes=[
            pltpu.VMEM((columns * atoms, 2 * channels), bf16),
            pltpu.VMEM((depth * tall, atoms), f32),
            pltpu.VMEM((atoms, CHUNK), f32),
            pltpu.VMEM((atoms, CHUNK), f32),
            pltpu.VMEM((GROUP * count, CHUNK), bf16),
            pltpu.VMEM((count, channels), f32),
            pltpu.VMEM((count, CHUNK), f32),
            pltpu.VMEM((atoms, channels), f32),
            pltpu.VMEM((depth, CHUNK, channels), bf16),
        ],
        cost_estimate=pl.CostEstimate(flops=40_000_000_000, transcendentals=0, bytes_accessed=2_000_000),
        name="conv",
    )
    most_rows = nx * ny * atoms + 2 * CHUNK
    ewald_call = lambda block: pl.pallas_call(
        functools.partial(ewald_body if block else ewald_first, depth, nx * ny * atoms, block),
        out_shape=jax.ShapeDtypeStruct((atoms, channels), bf16),
        in_specs=[vmem() for _ in range(8 if block else 7)],
        out_specs=vmem(),
        scratch_shapes=[
            pltpu.VMEM((3, waves, LANES), f32),
            pltpu.VMEM((2 * waves, LANES), bf16),
            pltpu.VMEM((2 * waves, CHUNK), bf16),
            pltpu.VMEM((2 * waves, channels), f32),
            pltpu.VMEM((waves, channels), f32),
            pltpu.VMEM((nx, ny * atoms, LANES), bf16),
            pltpu.VMEM((nx * (ny + -ny % 8), LANES), f32),
            pltpu.VMEM((most_rows, channels), f32),
            pltpu.VMEM((most_rows, LANES), f32),
            pltpu.VMEM((2, CHUNK, channels), bf16),
            pltpu.VMEM((2, 8, CHUNK), f32),
            pltpu.SMEM((nx,), jnp.int32),
            pltpu.SMEM((nx,), jnp.int32),
        ],
        cost_estimate=pl.CostEstimate(flops=30_000_000_000, transcendentals=0, bytes_accessed=4_000_000),
        name="ewald",
    )
    geo_planes = spread_out(payload)
    geo_all = jnp.stack(geo_planes)
    state_planes, state_all = geo_planes, geo_all
    for block in range(2):
        if block:
            state_planes = spread_out(state)
            state_all = jnp.stack(state_planes)
        conv = conv_call(block)(
            geo_planes[0],
            geo_planes[1],
            geo_planes[nx - 1],
            state_planes[0],
            state_planes[1],
            state_planes[nx - 1],
            input_weight,
            filter_weight,
            middle_weight,
            output_weight,
        )
        state = ewald_call(block)(
            wave_index,
            screening,
            geo_all,
            *([state_all] if block else []),
            state,
            conv,
            charge_weight,
            ewald_weight,
        )
    return state.reshape(features.shape)


def solution(mesh):
    in_specs = (
        P("gx", "gy", None, None),
        P("gx", "gy", None, None),
        P("gx", "gy", None),
        P(),
        P(),
        P(),
        P(),
        P(),
        P(),
        P(),
        P(),
    )
    out_specs = P("gx", "gy", None, None)
    return jax.shard_map(shards, mesh=mesh, in_specs=in_specs, out_specs=out_specs, check_vma=False)
```

```python
import functools
import math

import jax
import jax.numpy as jnp
from jax import lax
from jax.experimental import pallas as pl
from jax.experimental.pallas import tpu as pltpu
from jax.sharding import PartitionSpec as P


f32 = jnp.float32
bf16 = jnp.bfloat16

LANES = 128
GEO = 16
LIVE, LOW, SLOT, MID, SPOT = 3, 4, 7, 8, 11
CHUNK = 256
GROUP = 16
NONE = -1.0e30

COS_TURN = (
    1.0,
    -19.73920440673828,
    64.93911743164062,
    -85.45011138916016,
    60.16743087768555,
    -25.96688461303711,
    6.527706146240234,
)
SIN_TURN = (
    6.2831854820251465,
    -41.34170150756836,
    81.60513305664062,
    -76.7030029296875,
    42.02585220336914,
    -14.899578094482422,
    3.2377800941467285,
)
COS_HALF = (
    1.0,
    -1.2337005138397217,
    0.2536693215370178,
    -0.02086268737912178,
    0.000917722936719656,
    -2.3824151867302135e-05,
)


def power_sum(terms, x):
    out = terms[-1] * x + terms[-2]
    for term in terms[-3::-1]:
        out = out * x + term
    return out


def mm(a, b):
    return jnp.dot(a, b, preferred_element_type=f32)


def mm_nt(a, b):
    return lax.dot_general(a, b, (((1,), (1,)), ((), ())), preferred_element_type=f32)


def mm_tn(a, b):
    return lax.dot_general(a, b, (((0,), (0,)), ((), ())), preferred_element_type=f32)


def silu(t):
    return t / (1.0 + jnp.exp(-t))


def iota(shape, dim):
    return lax.broadcasted_iota(jnp.int32, shape, dim)


def vmem():
    return pl.BlockSpec(memory_space=pltpu.VMEM)


def smem():
    return pl.BlockSpec(memory_space=pltpu.SMEM)


def pack_kernel(counts_ref, features_ref, offsets_ref, out_ref):
    depth = counts_ref.shape[2]
    atoms, _ = features_ref.shape[2:]
    slots = atoms // depth
    out_ref[0:atoms, :] = features_ref[0, 0]
    lane = iota((1, atoms), 1)
    limit = jnp.zeros((1, atoms), jnp.int32)
    for cell in range(depth):
        limit = jnp.where(lane // slots == cell, counts_ref[0, 0, cell], limit)
    offset = offsets_ref[...]
    high = offset.astype(bf16).astype(f32)
    middle = (offset - high).astype(bf16).astype(f32)
    low = (offset - high) - middle
    rows = [high, (lane - (lane // slots) * slots < limit).astype(f32), low, (lane + 1).astype(f32), middle]
    rows.append(jnp.full((1, atoms), lax.axis_index("gx"), jnp.int32).astype(f32))
    rows.append(jnp.full((1, atoms), lax.axis_index("gy"), jnp.int32).astype(f32))
    rows.append((lane // slots).astype(f32))
    rows.append(jnp.zeros((2, atoms), f32))
    out_ref[atoms : atoms + GEO, :] = jnp.concatenate(rows, axis=0).astype(bf16)


def places(live, span):
    rows, atoms = live.shape
    before = (iota((atoms, atoms), 0) < iota((atoms, atoms), 1)).astype(f32).astype(bf16)
    live_b = live.astype(bf16)
    inside = mm(live_b, before)
    total = mm(live_b, jnp.ones((atoms, atoms), bf16))
    row, other = iota((rows, rows), 0), iota((rows, rows), 1)
    above = jnp.logical_and(other < row, other // span == row // span).astype(f32).astype(bf16)
    return jnp.where(live > 0.0, inside + mm(above, total.astype(bf16)), -1.0)


def chosen(place, first, size):
    want = (iota((size, place.shape[1]), 0) + first).astype(f32)
    return jnp.concatenate(
        [jnp.where(want == place[c : c + 1, :], 1.0, 0.0).astype(bf16) for c in range(place.shape[0])],
        axis=1,
    )


def identity(rows, columns):
    return (iota((rows, columns), 0) == iota((rows, columns), 1)).astype(f32).astype(bf16)


def joined(known, axis):
    high, middle, low = [known[axis + r : axis + r + 1] for r in (0, MID, LOW)]
    return (high + middle) + low


def grouped(known, groups):
    out = known[0:GEO]
    for g in range(1, groups):
        out = out + known[g * GEO : (g + 1) * GEO]
    return out


def wrapped(step, size):
    step = jnp.where(step > 0.5 * size, step - size, step)
    return jnp.where(step < -0.5 * size, step + size, step)


def outside(x):
    return jnp.maximum(jnp.maximum(-x, x - 1.0), 0.0)


def conv_kernel(
    depth,
    slots,
    size_x,
    size_y,
    rows_of,
    index,
    geo_a,
    geo_b,
    geo_c,
    state_a,
    state_b,
    state_c,
    input_ref,
    filter_ref,
    middle_ref,
    output_ref,
    out_ref,
    source_ref,
    place_ref,
    scale_ref,
    weight_ref,
    basis_ref,
    wide_ref,
    center_ref,
    message_ref,
    mapped_ref,
):
    atoms, channels = message_ref.shape
    count = filter_ref.shape[1]
    spread = math.sqrt(0.25 * math.log2(math.e))
    geo = (geo_a, geo_b, geo_c)
    state = (state_a, state_b, state_c)
    near = len(rows_of)
    columns = 3 * near
    block = columns + -columns % 8
    eye = identity(atoms, atoms)
    spots = [[], [], [], [], [], []]
    for plane in range(3):
        known = jnp.concatenate([geo[plane][row, atoms : atoms + GEO, :] for row in rows_of], axis=0)
        fill = jnp.zeros((channels - near * GEO, atoms), bf16)
        turned = mm_nt(eye, jnp.concatenate([known, fill], axis=0))
        group = iota(turned.shape, 1) // GEO
        wide = known.astype(f32)
        if plane == 0:
            here_x = wide[SPOT : SPOT + 1, 0:1]
            here_y = wide[SPOT + 1 : SPOT + 2, 0:1]
            target = [
                (turned[:, a : a + 1] + turned[:, MID + a : MID + a + 1]) + turned[:, LOW + a : LOW + a + 1]
                for a in range(3)
            ]
        for i, row in enumerate(rows_of):
            part = slice((plane * near + i) * atoms, (plane * near + i + 1) * atoms)
            source_ref[part, 0:channels] = mm(state[plane][row, 0:atoms, :], input_ref[index]).astype(bf16)
            source_ref[part, channels : 2 * channels] = jnp.where(group == i, turned, 0.0).astype(bf16)
            own = wide[i * GEO : (i + 1) * GEO]
            for a in range(3):
                spots[a].append(joined(own, a))
            for a, r in ((3, LIVE), (4, SPOT), (5, SPOT + 1)):
                spots[a].append(own[r : r + 1])
    fill = [jnp.zeros((block - columns, atoms), f32)]
    x, y, z, live, at_x, at_y = [jnp.concatenate(rows + fill, axis=0) for rows in spots]
    out_x = outside(wrapped(at_x - here_x, size_x) + x)
    out_y = outside(wrapped(at_y - here_y, size_y) + y)
    flat = out_x * out_x + out_y * out_y
    layers = (iota((block, atoms), 1) // slots).astype(f32)
    lives = []
    longest = jnp.int32(0)
    totals = []
    for cell in range(depth):
        out_z = outside(wrapped(layers - float(cell), depth) + z)
        close = jnp.where(flat + out_z * out_z < 1.001, live, 0.0)
        lives.append(close)
        totals.append(jnp.sum(close).astype(jnp.int32))
        longest = jnp.maximum(longest, totals[-1])
    place_ref[...] = places(jnp.concatenate(lives, axis=0), block)
    center_ref[...] = iota((count, CHUNK), 0).astype(f32) * spread
    wide_ref[...] = filter_ref[index].astype(f32)
    message_ref[...] = jnp.zeros_like(message_ref)
    pick_rows = identity(near * GEO, atoms)

    def piece(first, width):
        for cell in range(depth):
            want = chosen(place_ref[cell * block : cell * block + columns, :], first, width)
            found = mm(want, source_ref[...])
            mapped_ref[cell, 0:width, :] = found[:, 0:channels].astype(bf16)
            known = grouped(mm_nt(pick_rows, found[:, channels : 2 * channels].astype(bf16)), near)
            part = slice(cell * slots, (cell + 1) * slots)
            along_x = wrapped(known[SPOT : SPOT + 1] - here_x, size_x)
            along_y = wrapped(known[SPOT + 1 : SPOT + 2] - here_y, size_y)
            along_z = wrapped(known[SPOT + 2 : SPOT + 3] - float(cell), depth)
            home = jnp.abs(along_x) + jnp.abs(along_y)
            who = jnp.where(home == 0.0, known[SLOT : SLOT + 1], 0.0)
            diff_x = (along_x + joined(known, 0)) - target[0][part, :]
            diff_y = (along_y + joined(known, 1)) - target[1][part, :]
            diff_z = (along_z + joined(known, 2)) - target[2][part, :]
            square = diff_x * diff_x + diff_y * diff_y + diff_z * diff_z
            dist = jnp.sqrt(square)
            mine = (iota((slots, width), 0) + (cell * slots + 1)).astype(f32)
            kept = jnp.logical_and(dist < 1.0, who != mine)
            kept = jnp.logical_and(kept, iota((slots, width), 1) + first < totals[cell])
            half = jnp.maximum(power_sum(COS_HALF, jnp.minimum(square, 1.0)), 1.0e-18)
            weight_ref[part, 0:width] = jnp.where(kept, 2.0 * jnp.log2(half), NONE)
            scale_ref[part, 0:width] = dist * ((count - 1) * spread)

        def group_step(g, carry):
            start = pl.multiple_of(g * GROUP, GROUP)
            scale = scale_ref[pl.ds(start, GROUP), 0:width]
            weight = weight_ref[pl.ds(start, GROUP), 0:width]
            for i in range(GROUP):
                away = scale[i : i + 1, :] - center_ref[:, 0:width]
                basis_ref[i * count : (i + 1) * count, 0:width] = jnp.exp2(
                    weight[i : i + 1, :] - away * away
                ).astype(bf16)
            sums = mm(basis_ref[:, 0:width], mapped_ref[g // (slots // GROUP), 0:width, :])
            lines = []
            for i in range(GROUP):
                mixed = sums[i * count : (i + 1) * count, :] * wide_ref[...]
                lines.append(jnp.sum(mixed, axis=0, keepdims=True))
            message_ref[pl.ds(start, GROUP), :] += jnp.concatenate(lines, axis=0)
            return carry

        lax.fori_loop(0, atoms // GROUP, group_step, 0)

    full = (longest + (LANES - 1)) // CHUNK

    def chunk_step(chunk, carry):
        piece(chunk * CHUNK, CHUNK)
        return carry

    lax.fori_loop(0, full, chunk_step, 0)

    @pl.when(full * CHUNK < longest)
    def _():
        piece(full * CHUNK, LANES)

    middle = silu(mm(message_ref[...].astype(bf16), middle_ref[index])).astype(bf16)
    out_ref[...] = mm(middle, output_ref[index])


def phase_rows(wave_ref, x, y, z, put):
    waves = wave_ref.shape[1]
    step = 64
    for first in range(0, waves, step):
        part = slice(first, first + step)
        kx, ky, kz = [
            jnp.concatenate([wave_ref[a, part, :]] * (x.shape[1] // LANES), axis=1) for a in range(3)
        ]
        angle = kx * x + ky * y + kz * z
        rest = angle - jnp.round(angle)
        square = rest * rest
        put(first, power_sum(COS_TURN, square).astype(bf16))
        put(waves + first, (power_sum(SIN_TURN, square) * rest).astype(bf16))


def wave_columns(wave_ref, table_ref):
    waves = wave_ref.shape[1]
    eye = identity(LANES, LANES)
    numbers = jnp.concatenate([wave_ref[...].astype(f32), jnp.zeros((5, waves), f32)], axis=0).astype(bf16)
    for first in range(0, waves, LANES):
        turned = mm_nt(eye, numbers[:, first : first + LANES])
        for a in range(3):
            table_ref[a, first : first + LANES, :] = jnp.broadcast_to(turned[:, a : a + 1], (LANES, LANES))


def ewald_kernel(
    depth,
    total_atoms,
    index,
    keep,
    reuse,
    *refs,
):
    refs = list(refs)
    if reuse:
        base_ref = refs.pop(0)
        own_phase_ref, kept_ref = refs.pop(0), refs.pop(0)
        wave_ref, screen_ref, state_ref, own_ref, conv_ref, charge_ref, update_ref, out_ref = refs[:8]
        refs = refs[8:]
        planes, columns = state_ref.shape[0], state_ref.shape[1]
    else:
        wave_ref, screen_ref, geo_ref = refs[:3]
        refs = refs[3:]
        state_ref = geo_ref if index == 0 else refs.pop(0)
        own_ref, conv_ref, charge_ref, update_ref, out_ref = refs[:5]
        refs = refs[5:]
        if keep:
            base_out_ref, own_phase_ref, kept_ref = refs[:3]
            refs = refs[3:]
        else:
            own_phase_ref, base_out_ref = refs[:2]
            refs = refs[2:]
        base_ref, rows_ref, turned_ref, live_ref, packed_geo_ref, spot_ref, base_sem = refs[:7]
        refs = refs[7:]
        planes, columns = geo_ref.shape[0], geo_ref.shape[1]
    table_ref, phase_ref, factor_ref, damp_ref, packed_ref, tile_ref, phase_sem = refs
    atoms, channels = own_ref.shape
    slots = atoms // depth
    waves = wave_ref.shape[1]
    everyone = planes * columns
    wave_columns(wave_ref, table_ref)

    if not reuse:
        row = iota((3, 1), 0)
        unit = jnp.where(row == 0, 1.0 / planes, jnp.where(row == 1, 1.0 / columns, 1.0 / depth))

        def plane_rows(s, carry):
            spots, lives = [], []
            for t in range(columns):
                known = geo_ref[s, t, atoms : atoms + GEO, :].astype(f32)
                offset = (known[0:3] + known[MID : MID + 3]) + known[LOW : LOW + 3]
                spots += [(known[SPOT : SPOT + 3] + offset) * unit, jnp.zeros((1, atoms), f32)]
                lives.append(known[LIVE : LIVE + 1])
            tall = 4 * columns
            rows_ref[pl.ds(pl.multiple_of(s * tall, tall), tall), :] = jnp.concatenate(spots, axis=0)
            live_ref[pl.ds(pl.multiple_of(s * columns, columns), columns), :] = jnp.concatenate(lives, axis=0)
            return carry

        lax.fori_loop(0, planes, plane_rows, 0, unroll=4 if planes % 4 == 0 else 1)
        live = live_ref[...]
        before = (iota((atoms, atoms), 0) < iota((atoms, atoms), 1)).astype(f32).astype(bf16)
        live_b = live.astype(bf16)
        number = mm(live_b, jnp.ones((atoms, atoms), bf16))
        above = (iota((everyone, everyone), 1) < iota((everyone, everyone), 0)).astype(f32).astype(bf16)
        start = mm(above, number.astype(bf16))
        base_out_ref[0:everyone, :] = (mm(live_b, before) + start).astype(jnp.int32)
        last = (number + start)[everyone - 1 : everyone, :].astype(jnp.int32)
        base_out_ref[everyone : everyone + 8, :] = jnp.broadcast_to(last, (8, atoms))
        base_copy = pltpu.make_async_copy(base_out_ref, base_ref, base_sem)
        base_copy.start()
        for b in range(turned_ref.shape[0]):
            turned_ref[b] = rows_ref[b * LANES : (b + 1) * LANES, :].T
        own_rows = geo_ref[0, 0, atoms : atoms + GEO, :].astype(f32)
        offset = (own_rows[0:3] + own_rows[MID : MID + 3]) + own_rows[LOW : LOW + 3]
        own_spot = (own_rows[SPOT : SPOT + 3] + offset) * unit
        own_live = own_rows[LIVE : LIVE + 1].astype(bf16)

        def put_own(first, value):
            own_phase_ref[first : first + value.shape[0], :] = value * own_live

        phase_rows(table_ref, own_spot[0:1], own_spot[1:2], own_spot[2:3], put_own)

    full_turn = 6.283185307179586
    kx = table_ref[0] * (full_turn / planes)
    ky = table_ref[1] * (full_turn / columns)
    kz = table_ref[2] * (full_turn / depth)
    norm = 2.0 / math.sqrt(total_atoms)
    damp_ref[...] = norm * jnp.exp(-(kx * kx + ky * ky + kz * kz) / (4.0 * screen_ref[index : index + 1, :]))
    factor_ref[...] = jnp.zeros_like(factor_ref)
    if not reuse:
        base_copy.wait()
    total = base_ref[everyone, 0]
    pairs = (total + (CHUNK - 1)) // CHUNK

    def phase_copy(p, slot):
        if reuse:
            return pltpu.make_async_copy(kept_ref.at[p], phase_ref.at[slot], phase_sem.at[slot])
        return pltpu.make_async_copy(phase_ref.at[slot], kept_ref.at[p], phase_sem.at[slot])

    if reuse:
        phase_copy(0, 0).start()

    def pack_step(s, carry):
        for t in range(columns):
            c = s * columns + t
            for cell in range(depth):
                rows = pl.ds(base_ref[c, cell * slots], slots)
                part = slice(cell * slots, (cell + 1) * slots)
                packed_ref[rows, :] = state_ref[s, t, part, :].astype(f32)
                if not reuse:
                    spread = LANES // 4
                    mine = iota((slots, LANES), 1) // 4 == lax.rem(c, spread)
                    packed_geo_ref[rows, :] = jnp.where(mine, turned_ref[c // spread, part, :], 0.0)
        return carry

    lax.fori_loop(0, planes, pack_step, 0, unroll=2 if planes % 2 == 0 else 1)

    def prepare(p):
        rows = pl.ds(pl.multiple_of(p * CHUNK, CHUNK), CHUNK)
        slot = lax.rem(p, 2)
        valid = iota((CHUNK, channels), 0) + p * CHUNK < total
        picked = jnp.where(valid, packed_ref[rows, :], 0.0).astype(bf16)
        tile_ref[slot] = mm(picked, charge_ref[index]).astype(bf16)
        if not reuse:
            known = packed_geo_ref[rows, :].T
            known = jnp.sum(known.reshape(LANES // 8, 8, CHUNK), axis=0)
            known = known[0:4] + known[4:8]
            valid = iota((4, CHUNK), 1) + p * CHUNK < total
            spot_ref[slot, 0:4, :] = jnp.where(valid, known, 0.0)

    prepare(jnp.int32(0))

    def pair_step(p, carry):
        slot = lax.rem(p, 2)
        charge = tile_ref[slot]
        if reuse:

            @pl.when(p + 1 < pairs)
            def _():
                phase_copy(p + 1, 1 - slot).start()

            phase_copy(p, slot).wait()
        else:
            spot = spot_ref[slot]
            if keep:

                @pl.when(p >= 2)
                def _():
                    phase_copy(p - 2, slot).wait()

            def put(first, value):
                phase_ref[slot, first : first + value.shape[0], :] = value

            phase_rows(table_ref, spot[0:1], spot[1:2], spot[2:3], put)
        factor_ref[...] += mm(phase_ref[slot], charge)
        if keep and not reuse:
            phase_copy(p, slot).start()
        prepare(jnp.minimum(p + 1, pairs - 1))
        return carry

    lax.fori_loop(0, pairs, pair_step, 0)
    for side in range(2):
        part = slice(side * waves, (side + 1) * waves)
        factor_ref[part, :] = factor_ref[part, :] * damp_ref[...]
    damped = factor_ref[...].astype(bf16)
    field = mm_tn(own_phase_ref[...], damped)
    field = (field * (1.0 / math.sqrt(waves))).astype(bf16)
    ewald = silu(mm(field, update_ref[index]))
    out_ref[...] = (own_ref[...].astype(f32) + ewald + conv_ref[...]).astype(bf16)
    if keep and not reuse:

        @pl.when(pairs >= 2)
        def _():
            phase_copy(pairs - 2, lax.rem(pairs, 2)).wait()

        phase_copy(pairs - 1, lax.rem(pairs + 1, 2)).wait()


def gathered(rows, axis):
    size = lax.axis_size(axis)
    moved = [rows]
    near = [1, size - 1]
    for shift in near + list(range(2, size - 1)):
        moved.append(lax.ppermute(rows, axis, [(i, (i + shift) % size) for i in range(size)]))
    order = [0] + near + list(range(2, size - 1))
    return [moved[order.index(i)] for i in range(size)]


def shards(
    features,
    offsets,
    counts,
    wave_index,
    screening,
    charge_weight,
    ewald_weight,
    input_weight,
    filter_weight,
    middle_weight,
    output_weight,
):
    depth = counts.shape[2]
    atoms, channels = features.shape[2:]
    slots = atoms // depth
    nx = lax.axis_size("gx")
    ny = lax.axis_size("gy")
    waves = wave_index.shape[1]
    assert atoms == LANES and channels == LANES and waves % 64 == 0
    state = features.reshape(atoms, channels)
    payload = pl.pallas_call(
        pack_kernel,
        out_shape=jax.ShapeDtypeStruct((atoms + GEO, channels), bf16),
        in_specs=[smem(), vmem(), vmem()],
        out_specs=vmem(),
        name="pack",
    )(counts, features, offsets.reshape(3, atoms))

    rows_of = (0, 1, ny - 1)
    columns = 3 * len(rows_of)
    tall = columns + -columns % 8
    count = filter_weight.shape[1]

    def spread_out(rows):
        return gathered(jnp.stack(gathered(rows, "gy")), "gx")

    conv_call = lambda index: pl.pallas_call(
        functools.partial(conv_kernel, depth, slots, nx, ny, rows_of, index),
        out_shape=jax.ShapeDtypeStruct((atoms, channels), f32),
        in_specs=[vmem() for _ in range(10)],
        out_specs=vmem(),
        scratch_shapes=[
            pltpu.VMEM((columns * atoms, 2 * channels), bf16),
            pltpu.VMEM((depth * tall, atoms), f32),
            pltpu.VMEM((atoms, CHUNK), f32),
            pltpu.VMEM((atoms, CHUNK), f32),
            pltpu.VMEM((GROUP * count, CHUNK), bf16),
            pltpu.VMEM((count, channels), f32),
            pltpu.VMEM((count, CHUNK), f32),
            pltpu.VMEM((atoms, channels), f32),
            pltpu.VMEM((depth, CHUNK, channels), bf16),
        ],
        cost_estimate=pl.CostEstimate(flops=40_000_000_000, transcendentals=0, bytes_accessed=2_000_000),
        name="conv",
    )
    everyone = nx * ny
    most_pairs = -(-everyone * atoms // CHUNK)
    keep = most_pairs * 2 * waves * CHUNK * 2 <= 16 * 2**20
    most_rows = most_pairs * CHUNK + slots

    def ewald_call(index, *operands):
        reuse = keep and index > 0
        geometry = [] if reuse else [
            pltpu.SMEM((everyone + 8, atoms), jnp.int32),
            pltpu.VMEM((everyone * 4, LANES), f32),
            pltpu.VMEM((everyone * 4 // LANES, LANES, LANES), f32),
            pltpu.VMEM((everyone, atoms), f32),
            pltpu.VMEM((most_rows, LANES), f32),
            pltpu.VMEM((2, 8, CHUNK), f32),
            pltpu.SemaphoreType.DMA,
        ]
        own_phase, base = ((2 * waves, LANES), bf16), ((everyone + 8, atoms), jnp.int32)
        out_shape = [jax.ShapeDtypeStruct((atoms, channels), bf16)]
        out_specs = [vmem()]
        in_specs = [vmem() for _ in operands]
        hbm = pl.BlockSpec(memory_space=pl.ANY)
        if reuse:
            in_specs[0], in_specs[2] = smem(), hbm
        elif keep:
            out_shape += [jax.ShapeDtypeStruct(*base[:2]), jax.ShapeDtypeStruct(*own_phase[:2])]
            out_shape.append(jax.ShapeDtypeStruct((most_pairs, 2 * waves, CHUNK), bf16))
            out_specs += [vmem(), vmem(), hbm]
        else:
            geometry = [pltpu.VMEM(*own_phase), pltpu.VMEM(*base)] + geometry
        return pl.pallas_call(
            functools.partial(ewald_kernel, depth, everyone * atoms, index, keep, reuse),
            out_shape=out_shape,
            in_specs=in_specs,
            out_specs=out_specs,
            scratch_shapes=geometry
            + [
                pltpu.VMEM((3, waves, LANES), f32),
                pltpu.VMEM((2, 2 * waves, CHUNK), bf16),
                pltpu.VMEM((2 * waves, channels), f32),
                pltpu.VMEM((waves, channels), f32),
                pltpu.VMEM((most_rows, channels), f32),
                pltpu.VMEM((2, CHUNK, channels), bf16),
                pltpu.SemaphoreType.DMA((2,)),
            ],
            cost_estimate=pl.CostEstimate(flops=30_000_000_000, transcendentals=0, bytes_accessed=4_000_000),
            name="ewald",
        )(*operands)

    geo_planes = spread_out(payload)
    geo_all = jnp.stack(geo_planes)
    state_planes, state_all = geo_planes, geo_all
    for block in range(2):
        if block:
            state_planes = spread_out(state)
            state_all = jnp.stack(state_planes)
        conv = conv_call(block)(
            geo_planes[0],
            geo_planes[1],
            geo_planes[nx - 1],
            state_planes[0],
            state_planes[1],
            state_planes[nx - 1],
            input_weight,
            filter_weight,
            middle_weight,
            output_weight,
        )
        common = (state, conv, charge_weight, ewald_weight)
        if block == 0:
            state, *kept = ewald_call(block, wave_index, screening, geo_all, *common)
        elif keep:
            (state,) = ewald_call(block, *kept, wave_index, screening, state_all, *common)
        else:
            (state,) = ewald_call(block, wave_index, screening, geo_all, state_all, *common)
    return state.reshape(features.shape)


def solution(mesh):
    in_specs = (
        P("gx", "gy", None, None),
        P("gx", "gy", None, None),
        P("gx", "gy", None),
        P(),
        P(),
        P(),
        P(),
        P(),
        P(),
        P(),
        P(),
    )
    out_specs = P("gx", "gy", None, None)
    return jax.shard_map(shards, mesh=mesh, in_specs=in_specs, out_specs=out_specs, check_vma=False)
```

```python
import functools
import math

import jax
import jax.numpy as jnp
from jax import lax
from jax.experimental import pallas as pl
from jax.experimental.pallas import tpu as pltpu
from jax.sharding import PartitionSpec as P


f32 = jnp.float32
bf16 = jnp.bfloat16

LANES = 128
GEO = 16
LIVE, LOW, SLOT, MID, SPOT = 3, 4, 7, 8, 11
CHUNK = 256
GROUP = 16
NONE = -1.0e30
INPUT, FILTER, MIDDLE, OUTPUT = range(4)
AHEAD = 5

COS_TURN = (
    1.0,
    -19.73920440673828,
    64.93911743164062,
    -85.45011138916016,
    60.16743087768555,
    -25.96688461303711,
    6.527706146240234,
)
SIN_TURN = (
    6.2831854820251465,
    -41.34170150756836,
    81.60513305664062,
    -76.7030029296875,
    42.02585220336914,
    -14.899578094482422,
    3.2377800941467285,
)
COS_HALF = (
    1.0,
    -1.2337005138397217,
    0.2536693215370178,
    -0.02086268737912178,
    0.000917722936719656,
    -2.3824151867302135e-05,
)


def power_sum(terms, x):
    out = terms[-1] * x + terms[-2]
    for term in terms[-3::-1]:
        out = out * x + term
    return out


def mm(a, b):
    return jnp.dot(a, b, preferred_element_type=f32)


def mm_nt(a, b):
    return lax.dot_general(a, b, (((1,), (1,)), ((), ())), preferred_element_type=f32)


def mm_tn(a, b):
    return lax.dot_general(a, b, (((0,), (0,)), ((), ())), preferred_element_type=f32)


def silu(t):
    return t / (1.0 + jnp.exp(-t))


def iota(shape, dim):
    return lax.broadcasted_iota(jnp.int32, shape, dim)


def vmem():
    return pl.BlockSpec(memory_space=pltpu.VMEM)


def smem():
    return pl.BlockSpec(memory_space=pltpu.SMEM)


def pack_kernel(counts_ref, features_ref, offsets_ref, out_ref):
    depth = counts_ref.shape[2]
    atoms, _ = features_ref.shape[2:]
    slots = atoms // depth
    out_ref[0:atoms, :] = features_ref[0, 0]
    lane = iota((1, atoms), 1)
    limit = jnp.zeros((1, atoms), jnp.int32)
    for cell in range(depth):
        limit = jnp.where(lane // slots == cell, counts_ref[0, 0, cell], limit)
    offset = offsets_ref[...]
    high = offset.astype(bf16).astype(f32)
    middle = (offset - high).astype(bf16).astype(f32)
    low = (offset - high) - middle
    rows = [high, (lane - (lane // slots) * slots < limit).astype(f32), low, (lane + 1).astype(f32), middle]
    rows.append(jnp.full((1, atoms), lax.axis_index("gx"), jnp.int32).astype(f32))
    rows.append(jnp.full((1, atoms), lax.axis_index("gy"), jnp.int32).astype(f32))
    rows.append((lane // slots).astype(f32))
    rows.append(jnp.zeros((2, atoms), f32))
    out_ref[atoms : atoms + GEO, :] = jnp.concatenate(rows, axis=0).astype(bf16)


def places(live, span):
    rows, atoms = live.shape
    before = (iota((atoms, atoms), 0) < iota((atoms, atoms), 1)).astype(f32).astype(bf16)
    live_b = live.astype(bf16)
    inside = mm(live_b, before)
    total = mm(live_b, jnp.ones((atoms, atoms), bf16))
    row, other = iota((rows, rows), 0), iota((rows, rows), 1)
    above = jnp.logical_and(other < row, other // span == row // span).astype(f32).astype(bf16)
    return jnp.where(live > 0.0, inside + mm(above, total.astype(bf16)), -1.0)


def chosen(place, first, size):
    want = (iota((size, place.shape[1]), 0) + first).astype(f32)
    return jnp.concatenate(
        [jnp.where(want == place[c : c + 1, :], 1.0, 0.0).astype(bf16) for c in range(place.shape[0])],
        axis=1,
    )


def identity(rows, columns):
    return (iota((rows, columns), 0) == iota((rows, columns), 1)).astype(f32).astype(bf16)


def joined(known, axis):
    high, middle, low = [known[axis + r : axis + r + 1] for r in (0, MID, LOW)]
    return (high + middle) + low


def grouped(known, groups):
    out = known[0:GEO]
    for g in range(1, groups):
        out = out + known[g * GEO : (g + 1) * GEO]
    return out


def wrapped(step, size):
    step = jnp.where(step > 0.5 * size, step - size, step)
    return jnp.where(step < -0.5 * size, step + size, step)


def outside(x):
    return jnp.maximum(jnp.maximum(-x, x - 1.0), 0.0)


def conv_kernel(
    depth,
    slots,
    size_x,
    size_y,
    rows_of,
    index,
    geo_a,
    geo_b,
    geo_c,
    state_a,
    state_b,
    state_c,
    weight_all_ref,
    out_ref,
    source_ref,
    place_ref,
    scale_ref,
    weight_ref,
    basis_ref,
    wide_ref,
    center_ref,
    message_ref,
    mapped_ref,
):
    atoms, channels = message_ref.shape
    count = weight_all_ref.shape[1]
    input_at, filter_at, middle_at, output_at = [2 * kind + index for kind in (INPUT, FILTER, MIDDLE, OUTPUT)]
    spread = math.sqrt(0.25 * math.log2(math.e))
    geo = (geo_a, geo_b, geo_c)
    state = (state_a, state_b, state_c)
    near = len(rows_of)
    columns = 3 * near
    block = columns + -columns % 8
    eye = identity(atoms, atoms)
    spots = [[], [], [], [], [], []]
    for plane in range(3):
        known = jnp.concatenate([geo[plane][row, atoms : atoms + GEO, :] for row in rows_of], axis=0)
        fill = jnp.zeros((channels - near * GEO, atoms), bf16)
        turned = mm_nt(eye, jnp.concatenate([known, fill], axis=0))
        group = iota(turned.shape, 1) // GEO
        wide = known.astype(f32)
        if plane == 0:
            here_x = wide[SPOT : SPOT + 1, 0:1]
            here_y = wide[SPOT + 1 : SPOT + 2, 0:1]
            target = [
                (turned[:, a : a + 1] + turned[:, MID + a : MID + a + 1]) + turned[:, LOW + a : LOW + a + 1]
                for a in range(3)
            ]
        for i, row in enumerate(rows_of):
            part = slice((plane * near + i) * atoms, (plane * near + i + 1) * atoms)
            source_ref[part, 0:channels] = mm(state[plane][row, 0:atoms, :], weight_all_ref[input_at]).astype(bf16)
            source_ref[part, channels : 2 * channels] = jnp.where(group == i, turned, 0.0).astype(bf16)
            own = wide[i * GEO : (i + 1) * GEO]
            for a in range(3):
                spots[a].append(joined(own, a))
            for a, r in ((3, LIVE), (4, SPOT), (5, SPOT + 1)):
                spots[a].append(own[r : r + 1])
    fill = [jnp.zeros((block - columns, atoms), f32)]
    x, y, z, live, at_x, at_y = [jnp.concatenate(rows + fill, axis=0) for rows in spots]
    out_x = outside(wrapped(at_x - here_x, size_x) + x)
    out_y = outside(wrapped(at_y - here_y, size_y) + y)
    flat = out_x * out_x + out_y * out_y
    layers = (iota((block, atoms), 1) // slots).astype(f32)
    lives = []
    longest = jnp.int32(0)
    totals = []
    for cell in range(depth):
        out_z = outside(wrapped(layers - float(cell), depth) + z)
        close = jnp.where(flat + out_z * out_z < 1.001, live, 0.0)
        lives.append(close)
        totals.append(jnp.sum(close).astype(jnp.int32))
        longest = jnp.maximum(longest, totals[-1])
    place_ref[...] = places(jnp.concatenate(lives, axis=0), block)
    center_ref[...] = iota((count, CHUNK), 0).astype(f32) * spread
    wide_ref[...] = weight_all_ref[filter_at].astype(f32)
    message_ref[...] = jnp.zeros_like(message_ref)
    pick_rows = identity(near * GEO, atoms)

    def piece(first, width):
        for cell in range(depth):
            want = chosen(place_ref[cell * block : cell * block + columns, :], first, width)
            found = mm(want, source_ref[...])
            mapped_ref[cell, 0:width, :] = found[:, 0:channels].astype(bf16)
            known = grouped(mm_nt(pick_rows, found[:, channels : 2 * channels].astype(bf16)), near)
            part = slice(cell * slots, (cell + 1) * slots)
            along_x = wrapped(known[SPOT : SPOT + 1] - here_x, size_x)
            along_y = wrapped(known[SPOT + 1 : SPOT + 2] - here_y, size_y)
            along_z = wrapped(known[SPOT + 2 : SPOT + 3] - float(cell), depth)
            home = jnp.abs(along_x) + jnp.abs(along_y)
            who = jnp.where(home == 0.0, known[SLOT : SLOT + 1], 0.0)
            diff_x = (along_x + joined(known, 0)) - target[0][part, :]
            diff_y = (along_y + joined(known, 1)) - target[1][part, :]
            diff_z = (along_z + joined(known, 2)) - target[2][part, :]
            square = diff_x * diff_x + diff_y * diff_y + diff_z * diff_z
            dist = jnp.sqrt(square)
            mine = (iota((slots, width), 0) + (cell * slots + 1)).astype(f32)
            kept = jnp.logical_and(dist < 1.0, who != mine)
            kept = jnp.logical_and(kept, iota((slots, width), 1) + first < totals[cell])
            half = jnp.maximum(power_sum(COS_HALF, jnp.minimum(square, 1.0)), 1.0e-18)
            weight_ref[part, 0:width] = jnp.where(kept, 2.0 * jnp.log2(half), NONE)
            scale_ref[part, 0:width] = dist * ((count - 1) * spread)

        def group_step(g, carry):
            start = pl.multiple_of(g * GROUP, GROUP)
            scale = scale_ref[pl.ds(start, GROUP), 0:width]
            weight = weight_ref[pl.ds(start, GROUP), 0:width]
            for i in range(GROUP):
                away = scale[i : i + 1, :] - center_ref[:, 0:width]
                basis_ref[i * count : (i + 1) * count, 0:width] = jnp.exp2(
                    weight[i : i + 1, :] - away * away
                ).astype(bf16)
            sums = mm(basis_ref[:, 0:width], mapped_ref[g // (slots // GROUP), 0:width, :])
            lines = []
            for i in range(GROUP):
                mixed = sums[i * count : (i + 1) * count, :] * wide_ref[...]
                lines.append(jnp.sum(mixed, axis=0, keepdims=True))
            message_ref[pl.ds(start, GROUP), :] += jnp.concatenate(lines, axis=0)
            return carry

        lax.fori_loop(0, atoms // GROUP, group_step, 0)

    full = (longest + (LANES - 1)) // CHUNK

    def chunk_step(chunk, carry):
        piece(chunk * CHUNK, CHUNK)
        return carry

    lax.fori_loop(0, full, chunk_step, 0)

    @pl.when(full * CHUNK < longest)
    def _():
        piece(full * CHUNK, LANES)

    middle = silu(mm(message_ref[...].astype(bf16), weight_all_ref[middle_at])).astype(bf16)
    out_ref[...] = mm(middle, weight_all_ref[output_at])


def phase_rows(wave_ref, x, y, z, put):
    waves = wave_ref.shape[1]
    step = 64
    for first in range(0, waves, step):
        part = slice(first, first + step)
        kx, ky, kz = [
            jnp.concatenate([wave_ref[a, part, :]] * (x.shape[1] // LANES), axis=1) for a in range(3)
        ]
        angle = kx * x + ky * y + kz * z
        rest = angle - jnp.round(angle)
        square = rest * rest
        put(first, power_sum(COS_TURN, square).astype(bf16))
        put(waves + first, (power_sum(SIN_TURN, square) * rest).astype(bf16))


def wave_columns(wave_ref, table_ref):
    waves = wave_ref.shape[1]
    eye = identity(LANES, LANES)
    numbers = jnp.concatenate([wave_ref[...].astype(f32), jnp.zeros((5, waves), f32)], axis=0).astype(bf16)
    for first in range(0, waves, LANES):
        turned = mm_nt(eye, numbers[:, first : first + LANES])
        for a in range(3):
            table_ref[a, first : first + LANES, :] = jnp.broadcast_to(turned[:, a : a + 1], (LANES, LANES))


def ewald_kernel(
    depth,
    total_atoms,
    index,
    keep,
    reuse,
    *refs,
):
    refs = list(refs)
    if reuse:
        base_ref = refs.pop(0)
        own_phase_ref, kept_ref = refs.pop(0), refs.pop(0)
        wave_ref, screen_ref, state_ref, own_ref, conv_ref, charge_ref, update_ref, out_ref = refs[:8]
        refs = refs[8:]
        planes, columns = state_ref.shape[0], state_ref.shape[1]
    else:
        wave_ref, screen_ref, geo_ref = refs[:3]
        refs = refs[3:]
        state_ref = geo_ref if index == 0 else refs.pop(0)
        own_ref, conv_ref, charge_ref, update_ref, out_ref = refs[:5]
        refs = refs[5:]
        if keep:
            base_out_ref, own_phase_ref, kept_ref = refs[:3]
            refs = refs[3:]
        else:
            own_phase_ref, base_out_ref = refs[:2]
            refs = refs[2:]
        base_ref, rows_ref, turned_ref, live_ref, packed_geo_ref, spot_ref, base_sem = refs[:7]
        refs = refs[7:]
        planes, columns = geo_ref.shape[0], geo_ref.shape[1]
    table_ref, phase_ref, factor_ref, damp_ref, packed_ref, tile_ref, phase_sem = refs
    atoms, channels = own_ref.shape
    slots = atoms // depth
    waves = wave_ref.shape[1]
    everyone = planes * columns
    wave_columns(wave_ref, table_ref)

    if not reuse:
        row = iota((3, 1), 0)
        unit = jnp.where(row == 0, 1.0 / planes, jnp.where(row == 1, 1.0 / columns, 1.0 / depth))

        def plane_rows(s, carry):
            spots, lives = [], []
            for t in range(columns):
                known = geo_ref[s, t, atoms : atoms + GEO, :].astype(f32)
                offset = (known[0:3] + known[MID : MID + 3]) + known[LOW : LOW + 3]
                spots += [(known[SPOT : SPOT + 3] + offset) * unit, jnp.zeros((1, atoms), f32)]
                lives.append(known[LIVE : LIVE + 1])
            tall = 4 * columns
            rows_ref[pl.ds(pl.multiple_of(s * tall, tall), tall), :] = jnp.concatenate(spots, axis=0)
            live_ref[pl.ds(pl.multiple_of(s * columns, columns), columns), :] = jnp.concatenate(lives, axis=0)
            return carry

        lax.fori_loop(0, planes, plane_rows, 0, unroll=4 if planes % 4 == 0 else 1)
        live = live_ref[...]
        before = (iota((atoms, atoms), 0) < iota((atoms, atoms), 1)).astype(f32).astype(bf16)
        live_b = live.astype(bf16)
        number = mm(live_b, jnp.ones((atoms, atoms), bf16))
        above = (iota((everyone, everyone), 1) < iota((everyone, everyone), 0)).astype(f32).astype(bf16)
        start = mm(above, number.astype(bf16))
        base_out_ref[0:everyone, :] = (mm(live_b, before) + start).astype(jnp.int32)
        last = (number + start)[everyone - 1 : everyone, :].astype(jnp.int32)
        base_out_ref[everyone : everyone + 8, :] = jnp.broadcast_to(last, (8, atoms))
        base_copy = pltpu.make_async_copy(base_out_ref, base_ref, base_sem)
        base_copy.start()
        for b in range(turned_ref.shape[0]):
            turned_ref[b] = rows_ref[b * LANES : (b + 1) * LANES, :].T
        own_rows = geo_ref[0, 0, atoms : atoms + GEO, :].astype(f32)
        offset = (own_rows[0:3] + own_rows[MID : MID + 3]) + own_rows[LOW : LOW + 3]
        own_spot = (own_rows[SPOT : SPOT + 3] + offset) * unit
        own_live = own_rows[LIVE : LIVE + 1].astype(bf16)

        def put_own(first, value):
            own_phase_ref[first : first + value.shape[0], :] = value * own_live

        phase_rows(table_ref, own_spot[0:1], own_spot[1:2], own_spot[2:3], put_own)

    full_turn = 6.283185307179586
    kx = table_ref[0] * (full_turn / planes)
    ky = table_ref[1] * (full_turn / columns)
    kz = table_ref[2] * (full_turn / depth)
    norm = 2.0 / math.sqrt(total_atoms)
    damp_ref[...] = norm * jnp.exp(-(kx * kx + ky * ky + kz * kz) / (4.0 * screen_ref[index : index + 1, :]))
    factor_ref[...] = jnp.zeros_like(factor_ref)
    if not reuse:
        base_copy.wait()
    total = base_ref[everyone, 0]
    pairs = (total + (CHUNK - 1)) // CHUNK

    def phase_copy(p, slot):
        if reuse:
            return pltpu.make_async_copy(kept_ref.at[p], phase_ref.at[slot], phase_sem.at[slot])
        return pltpu.make_async_copy(phase_ref.at[slot], kept_ref.at[p], phase_sem.at[slot])

    if reuse:
        for p in range(AHEAD - 1):

            @pl.when(p < pairs)
            def _(p=p):
                phase_copy(p, p).start()

    def pack_step(s, carry):
        for t in range(columns):
            c = s * columns + t
            for cell in range(depth):
                rows = pl.ds(base_ref[c, cell * slots], slots)
                part = slice(cell * slots, (cell + 1) * slots)
                packed_ref[rows, :] = state_ref[s, t, part, :].astype(f32)
                if not reuse:
                    spread = LANES // 4
                    mine = iota((slots, LANES), 1) // 4 == lax.rem(c, spread)
                    packed_geo_ref[rows, :] = jnp.where(mine, turned_ref[c // spread, part, :], 0.0)
        return carry

    lax.fori_loop(0, planes, pack_step, 0, unroll=2 if planes % 2 == 0 else 1)

    def prepare(p):
        rows = pl.ds(pl.multiple_of(p * CHUNK, CHUNK), CHUNK)
        slot = lax.rem(p, 2)
        valid = iota((CHUNK, channels), 0) + p * CHUNK < total
        picked = jnp.where(valid, packed_ref[rows, :], 0.0).astype(bf16)
        tile_ref[slot] = mm(picked, charge_ref[index]).astype(bf16)
        if not reuse:
            known = packed_geo_ref[rows, :].T
            known = jnp.sum(known.reshape(LANES // 8, 8, CHUNK), axis=0)
            known = known[0:4] + known[4:8]
            valid = iota((4, CHUNK), 1) + p * CHUNK < total
            spot_ref[slot, 0:4, :] = jnp.where(valid, known, 0.0)

    prepare(jnp.int32(0))

    def pair_step(p, carry):
        slot = lax.rem(p, 2)
        charge = tile_ref[slot]
        if reuse:

            ring = lax.rem(p, AHEAD)

            @pl.when(p + AHEAD - 1 < pairs)
            def _():
                phase_copy(p + AHEAD - 1, lax.rem(p + AHEAD - 1, AHEAD)).start()

            phase_copy(p, ring).wait()
        else:
            ring = slot
            spot = spot_ref[slot]
            if keep:

                @pl.when(p >= 2)
                def _():
                    phase_copy(p - 2, slot).wait()

            def put(first, value):
                phase_ref[slot, first : first + value.shape[0], :] = value

            phase_rows(table_ref, spot[0:1], spot[1:2], spot[2:3], put)
        factor_ref[...] += mm(phase_ref[ring], charge)
        if keep and not reuse:
            phase_copy(p, slot).start()
        prepare(jnp.minimum(p + 1, pairs - 1))
        return carry

    lax.fori_loop(0, pairs, pair_step, 0)
    for side in range(2):
        part = slice(side * waves, (side + 1) * waves)
        factor_ref[part, :] = factor_ref[part, :] * damp_ref[...]
    damped = factor_ref[...].astype(bf16)
    field = mm_tn(own_phase_ref[...], damped)
    field = (field * (1.0 / math.sqrt(waves))).astype(bf16)
    ewald = silu(mm(field, update_ref[index]))
    out_ref[...] = (own_ref[...].astype(f32) + ewald + conv_ref[...]).astype(bf16)
    if keep and not reuse:

        @pl.when(pairs >= 2)
        def _():
            phase_copy(pairs - 2, lax.rem(pairs, 2)).wait()

        phase_copy(pairs - 1, lax.rem(pairs + 1, 2)).wait()


def gathered(rows, axis):
    size = lax.axis_size(axis)
    moved = [rows]
    near = [1, size - 1]
    for shift in near + list(range(2, size - 1)):
        moved.append(lax.ppermute(rows, axis, [(i, (i + shift) % size) for i in range(size)]))
    order = [0] + near + list(range(2, size - 1))
    return [moved[order.index(i)] for i in range(size)]


def shards(
    features,
    offsets,
    counts,
    wave_index,
    screening,
    charge_weight,
    ewald_weight,
    input_weight,
    filter_weight,
    middle_weight,
    output_weight,
):
    depth = counts.shape[2]
    atoms, channels = features.shape[2:]
    slots = atoms // depth
    nx = lax.axis_size("gx")
    ny = lax.axis_size("gy")
    waves = wave_index.shape[1]
    assert atoms == channels == filter_weight.shape[1] == LANES and waves % 64 == 0
    state = features.reshape(atoms, channels)
    weights = jnp.concatenate([input_weight, filter_weight, middle_weight, output_weight], axis=0)
    payload = pl.pallas_call(
        pack_kernel,
        out_shape=jax.ShapeDtypeStruct((atoms + GEO, channels), bf16),
        in_specs=[smem(), vmem(), vmem()],
        out_specs=vmem(),
        compiler_params=pltpu.CompilerParams(vmem_limit_bytes=4 * 2**20),
        name="pack",
    )(counts, features, offsets.reshape(3, atoms))

    rows_of = (0, 1, ny - 1)
    columns = 3 * len(rows_of)
    tall = columns + -columns % 8
    count = filter_weight.shape[1]

    def spread_out(rows):
        return gathered(jnp.stack(gathered(rows, "gy")), "gx")

    conv_call = lambda index: pl.pallas_call(
        functools.partial(conv_kernel, depth, slots, nx, ny, rows_of, index),
        out_shape=jax.ShapeDtypeStruct((atoms, channels), f32),
        in_specs=[vmem() for _ in range(7)],
        out_specs=vmem(),
        scratch_shapes=[
            pltpu.VMEM((columns * atoms, 2 * channels), bf16),
            pltpu.VMEM((depth * tall, atoms), f32),
            pltpu.VMEM((atoms, CHUNK), f32),
            pltpu.VMEM((atoms, CHUNK), f32),
            pltpu.VMEM((GROUP * count, CHUNK), bf16),
            pltpu.VMEM((count, channels), f32),
            pltpu.VMEM((count, CHUNK), f32),
            pltpu.VMEM((atoms, channels), f32),
            pltpu.VMEM((depth, CHUNK, channels), bf16),
        ],
        compiler_params=pltpu.CompilerParams(vmem_limit_bytes=16 * 2**20),
        cost_estimate=pl.CostEstimate(flops=40_000_000_000, transcendentals=0, bytes_accessed=2_000_000),
        name="conv",
    )
    everyone = nx * ny
    most_pairs = -(-everyone * atoms // CHUNK)
    keep = most_pairs * 2 * waves * CHUNK * 2 <= 16 * 2**20
    most_rows = most_pairs * CHUNK + slots
    room = min((12 + everyone // 3) * 2**20, 60 * 2**20)

    def ewald_call(index, *operands):
        reuse = keep and index > 0
        geometry = [] if reuse else [
            pltpu.SMEM((everyone + 8, atoms), jnp.int32),
            pltpu.VMEM((everyone * 4, LANES), f32),
            pltpu.VMEM((everyone * 4 // LANES, LANES, LANES), f32),
            pltpu.VMEM((everyone, atoms), f32),
            pltpu.VMEM((most_rows, LANES), f32),
            pltpu.VMEM((2, 8, CHUNK), f32),
            pltpu.SemaphoreType.DMA,
        ]
        own_phase, base = ((2 * waves, LANES), bf16), ((everyone + 8, atoms), jnp.int32)
        out_shape = [jax.ShapeDtypeStruct((atoms, channels), bf16)]
        out_specs = [vmem()]
        in_specs = [vmem() for _ in operands]
        hbm = pl.BlockSpec(memory_space=pl.ANY)
        if reuse:
            in_specs[0], in_specs[2] = smem(), hbm
        elif keep:
            out_shape += [jax.ShapeDtypeStruct(*base[:2]), jax.ShapeDtypeStruct(*own_phase[:2])]
            out_shape.append(jax.ShapeDtypeStruct((most_pairs, 2 * waves, CHUNK), bf16))
            out_specs += [vmem(), vmem(), hbm]
        else:
            geometry = [pltpu.VMEM(*own_phase), pltpu.VMEM(*base)] + geometry
        return pl.pallas_call(
            functools.partial(ewald_kernel, depth, everyone * atoms, index, keep, reuse),
            out_shape=out_shape,
            in_specs=in_specs,
            out_specs=out_specs,
            scratch_shapes=geometry
            + [
                pltpu.VMEM((3, waves, LANES), f32),
                pltpu.VMEM((AHEAD if reuse else 2, 2 * waves, CHUNK), bf16),
                pltpu.VMEM((2 * waves, channels), f32),
                pltpu.VMEM((waves, channels), f32),
                pltpu.VMEM((most_rows, channels), f32),
                pltpu.VMEM((2, CHUNK, channels), bf16),
                pltpu.SemaphoreType.DMA((AHEAD if reuse else 2,)),
            ],
            compiler_params=pltpu.CompilerParams(vmem_limit_bytes=room),
            cost_estimate=pl.CostEstimate(flops=30_000_000_000, transcendentals=0, bytes_accessed=4_000_000),
            name="ewald",
        )(*operands)

    geo_planes = spread_out(payload)
    geo_all = jnp.stack(geo_planes)
    state_planes, state_all = geo_planes, geo_all
    for block in range(2):
        if block:
            state_planes = spread_out(state)
            state_all = jnp.stack(state_planes)
        conv = conv_call(block)(
            geo_planes[0],
            geo_planes[1],
            geo_planes[nx - 1],
            state_planes[0],
            state_planes[1],
            state_planes[nx - 1],
            weights,
        )
        common = (state, conv, charge_weight, ewald_weight)
        if block == 0:
            state, *kept = ewald_call(block, wave_index, screening, geo_all, *common)
        elif keep:
            (state,) = ewald_call(block, *kept, wave_index, screening, state_all, *common)
        else:
            (state,) = ewald_call(block, wave_index, screening, geo_all, state_all, *common)
    return state.reshape(features.shape)


def solution(mesh):
    in_specs = (
        P("gx", "gy", None, None),
        P("gx", "gy", None, None),
        P("gx", "gy", None),
        P(),
        P(),
        P(),
        P(),
        P(),
        P(),
        P(),
        P(),
    )
    out_specs = P("gx", "gy", None, None)
    return jax.shard_map(shards, mesh=mesh, in_specs=in_specs, out_specs=out_specs, check_vma=False)
```

```python
import functools
import math

import jax
import jax.numpy as jnp
from jax import lax
from jax.experimental import pallas as pl
from jax.experimental.pallas import tpu as pltpu
from jax.sharding import PartitionSpec as P


f32 = jnp.float32
bf16 = jnp.bfloat16

LANES = 128
GEO = 16
LIVE, LOW, SLOT, MID, SPOT = 3, 4, 7, 8, 11
CHUNK = 256
WIDE = 384
GROUP = 16
NONE = -1.0e30
INPUT, FILTER, MIDDLE, OUTPUT = range(4)
AHEAD = 5

COS_TURN = (
    1.0,
    -19.73920440673828,
    64.93911743164062,
    -85.45011138916016,
    60.16743087768555,
    -25.96688461303711,
    6.527706146240234,
)
SIN_TURN = (
    6.2831854820251465,
    -41.34170150756836,
    81.60513305664062,
    -76.7030029296875,
    42.02585220336914,
    -14.899578094482422,
    3.2377800941467285,
)
COS_HALF = (
    1.0,
    -1.2337005138397217,
    0.2536693215370178,
    -0.02086268737912178,
    0.000917722936719656,
    -2.3824151867302135e-05,
)


def power_sum(terms, x):
    out = terms[-1] * x + terms[-2]
    for term in terms[-3::-1]:
        out = out * x + term
    return out


def mm(a, b):
    return jnp.dot(a, b, preferred_element_type=f32)


def mm_nt(a, b):
    return lax.dot_general(a, b, (((1,), (1,)), ((), ())), preferred_element_type=f32)


def mm_tn(a, b):
    return lax.dot_general(a, b, (((0,), (0,)), ((), ())), preferred_element_type=f32)


def silu(t):
    return t / (1.0 + jnp.exp(-t))


def iota(shape, dim):
    return lax.broadcasted_iota(jnp.int32, shape, dim)


def vmem():
    return pl.BlockSpec(memory_space=pltpu.VMEM)


def smem():
    return pl.BlockSpec(memory_space=pltpu.SMEM)


def pack_kernel(counts_ref, features_ref, offsets_ref, out_ref):
    depth = counts_ref.shape[2]
    atoms, _ = features_ref.shape[2:]
    slots = atoms // depth
    out_ref[0:atoms, :] = features_ref[0, 0]
    lane = iota((1, atoms), 1)
    limit = jnp.zeros((1, atoms), jnp.int32)
    for cell in range(depth):
        limit = jnp.where(lane // slots == cell, counts_ref[0, 0, cell], limit)
    offset = offsets_ref[...]
    high = offset.astype(bf16).astype(f32)
    middle = (offset - high).astype(bf16).astype(f32)
    low = (offset - high) - middle
    rows = [high, (lane - (lane // slots) * slots < limit).astype(f32), low, (lane + 1).astype(f32), middle]
    rows.append(jnp.full((1, atoms), lax.axis_index("gx"), jnp.int32).astype(f32))
    rows.append(jnp.full((1, atoms), lax.axis_index("gy"), jnp.int32).astype(f32))
    rows.append((lane // slots).astype(f32))
    rows.append(jnp.zeros((2, atoms), f32))
    out_ref[atoms : atoms + GEO, :] = jnp.concatenate(rows, axis=0).astype(bf16)


def places(live, span):
    rows, atoms = live.shape
    before = (iota((atoms, atoms), 0) < iota((atoms, atoms), 1)).astype(f32).astype(bf16)
    live_b = live.astype(bf16)
    inside = mm(live_b, before)
    total = mm(live_b, jnp.ones((atoms, atoms), bf16))
    row, other = iota((rows, rows), 0), iota((rows, rows), 1)
    above = jnp.logical_and(other < row, other // span == row // span).astype(f32).astype(bf16)
    return jnp.where(live > 0.0, inside + mm(above, total.astype(bf16)), -1.0)


def chosen(place, first, size):
    want = (iota((size, place.shape[1]), 0) + first).astype(f32)
    return jnp.concatenate(
        [jnp.where(want == place[c : c + 1, :], 1.0, 0.0).astype(bf16) for c in range(place.shape[0])],
        axis=1,
    )


def identity(rows, columns):
    return (iota((rows, columns), 0) == iota((rows, columns), 1)).astype(f32).astype(bf16)


def joined(known, axis):
    high, middle, low = [known[axis + r : axis + r + 1] for r in (0, MID, LOW)]
    return (high + middle) + low


def grouped(known, groups):
    out = known[0:GEO]
    for g in range(1, groups):
        out = out + known[g * GEO : (g + 1) * GEO]
    return out


def wrapped(step, size):
    step = jnp.where(step > 0.5 * size, step - size, step)
    return jnp.where(step < -0.5 * size, step + size, step)


def outside(x):
    return jnp.maximum(jnp.maximum(-x, x - 1.0), 0.0)


def conv_kernel(
    depth,
    slots,
    size_x,
    size_y,
    rows_of,
    index,
    geo_a,
    geo_b,
    geo_c,
    state_a,
    state_b,
    state_c,
    weight_all_ref,
    out_ref,
    source_ref,
    place_ref,
    scale_ref,
    weight_ref,
    basis_ref,
    wide_ref,
    center_ref,
    message_ref,
    mapped_ref,
    target_ref,
    total_ref,
):
    atoms, channels = message_ref.shape
    count = weight_all_ref.shape[1]
    input_at, filter_at, middle_at, output_at = [2 * kind + index for kind in (INPUT, FILTER, MIDDLE, OUTPUT)]
    spread = math.sqrt(0.25 * math.log2(math.e))
    geo = (geo_a, geo_b, geo_c)
    state = (state_a, state_b, state_c)
    near = len(rows_of)
    columns = 3 * near
    block = columns + -columns % 8
    eye = identity(atoms, atoms)
    spots = [[], [], [], [], [], []]
    for plane in range(3):
        known = jnp.concatenate([geo[plane][row, atoms : atoms + GEO, :] for row in rows_of], axis=0)
        fill = jnp.zeros((channels - near * GEO, atoms), bf16)
        turned = mm_nt(eye, jnp.concatenate([known, fill], axis=0))
        group = iota(turned.shape, 1) // GEO
        wide = known.astype(f32)
        if plane == 0:
            here_x = wide[SPOT : SPOT + 1, 0:1]
            here_y = wide[SPOT + 1 : SPOT + 2, 0:1]
            for a in range(3):
                target_ref[:, a : a + 1] = (
                    turned[:, a : a + 1] + turned[:, MID + a : MID + a + 1]
                ) + turned[:, LOW + a : LOW + a + 1]
        for i, row in enumerate(rows_of):
            part = slice((plane * near + i) * atoms, (plane * near + i + 1) * atoms)
            source_ref[part, 0:channels] = mm(state[plane][row, 0:atoms, :], weight_all_ref[input_at]).astype(bf16)
            source_ref[part, channels : 2 * channels] = jnp.where(group == i, turned, 0.0).astype(bf16)
            own = wide[i * GEO : (i + 1) * GEO]
            for a in range(3):
                spots[a].append(joined(own, a))
            for a, r in ((3, LIVE), (4, SPOT), (5, SPOT + 1)):
                spots[a].append(own[r : r + 1])
    fill = [jnp.zeros((block - columns, atoms), f32)]
    x, y, z, live, at_x, at_y = [jnp.concatenate(rows + fill, axis=0) for rows in spots]
    out_x = outside(wrapped(at_x - here_x, size_x) + x)
    out_y = outside(wrapped(at_y - here_y, size_y) + y)
    flat = out_x * out_x + out_y * out_y
    layers = (iota((block, atoms), 1) // slots).astype(f32)
    lives = []
    longest = jnp.int32(0)
    for cell in range(depth):
        out_z = outside(wrapped(layers - float(cell), depth) + z)
        close = jnp.where(flat + out_z * out_z < 1.001, live, 0.0)
        lives.append(close)
        total = jnp.sum(close).astype(jnp.int32)
        total_ref[cell] = total
        longest = jnp.maximum(longest, total)
    place_ref[...] = places(jnp.concatenate(lives, axis=0), block)
    center_ref[...] = iota((count, WIDE), 0).astype(f32) * spread
    wide_ref[...] = weight_all_ref[filter_at].astype(f32)
    message_ref[...] = jnp.zeros_like(message_ref)
    pick_rows = identity(near * GEO, atoms)

    def piece(first, width):
        def cell_step(cell, carry):
            rows = pl.ds(pl.multiple_of(cell * block, block), block)
            want = chosen(place_ref[rows, :][0:columns], first, width)
            found = mm(want, source_ref[...])
            mapped_ref[cell, 0:width, :] = found[:, 0:channels].astype(bf16)
            known = grouped(mm_nt(pick_rows, found[:, channels : 2 * channels].astype(bf16)), near)
            part = pl.ds(pl.multiple_of(cell * slots, slots), slots)
            along_x = wrapped(known[SPOT : SPOT + 1] - here_x, size_x)
            along_y = wrapped(known[SPOT + 1 : SPOT + 2] - here_y, size_y)
            along_z = wrapped(known[SPOT + 2 : SPOT + 3] - cell.astype(f32), depth)
            home = jnp.abs(along_x) + jnp.abs(along_y)
            who = jnp.where(home == 0.0, known[SLOT : SLOT + 1], 0.0)
            target = target_ref[part, :]
            diff_x = (along_x + joined(known, 0)) - target[:, 0:1]
            diff_y = (along_y + joined(known, 1)) - target[:, 1:2]
            diff_z = (along_z + joined(known, 2)) - target[:, 2:3]
            square = diff_x * diff_x + diff_y * diff_y + diff_z * diff_z
            dist = jnp.sqrt(square)
            mine = (iota((slots, width), 0) + (cell * slots + 1)).astype(f32)
            kept = jnp.logical_and(dist < 1.0, who != mine)
            kept = jnp.logical_and(kept, iota((slots, width), 1) + first < total_ref[cell])
            half = jnp.maximum(power_sum(COS_HALF, jnp.minimum(square, 1.0)), 1.0e-18)
            weight_ref[part, 0:width] = jnp.where(kept, 2.0 * jnp.log2(half), NONE)
            scale_ref[part, 0:width] = dist * ((count - 1) * spread)
            return carry

        lax.fori_loop(0, depth, cell_step, 0)

        def group_step(g, carry):
            start = pl.multiple_of(g * GROUP, GROUP)
            scale = scale_ref[pl.ds(start, GROUP), 0:width]
            weight = weight_ref[pl.ds(start, GROUP), 0:width]
            for i in range(GROUP):
                away = scale[i : i + 1, :] - center_ref[:, 0:width]
                basis_ref[i * count : (i + 1) * count, 0:width] = jnp.exp2(
                    weight[i : i + 1, :] - away * away
                ).astype(bf16)
            sums = mm(basis_ref[:, 0:width], mapped_ref[g // (slots // GROUP), 0:width, :])
            lines = []
            for i in range(GROUP):
                mixed = sums[i * count : (i + 1) * count, :] * wide_ref[...]
                lines.append(jnp.sum(mixed, axis=0, keepdims=True))
            message_ref[pl.ds(start, GROUP), :] += jnp.concatenate(lines, axis=0)
            return carry

        lax.fori_loop(0, atoms // GROUP, group_step, 0)

    tiles = (longest + (LANES - 1)) // LANES
    odd = jnp.logical_and(lax.rem(tiles, 2) == 1, tiles >= 3)
    full = (tiles + 1) // 2 - jnp.where(odd, 2, 0)

    def chunk_step(chunk, carry):
        piece(chunk * CHUNK, CHUNK)
        return carry

    lax.fori_loop(0, full, chunk_step, 0)

    @pl.when(odd)
    def _():
        piece(full * CHUNK, WIDE)

    middle = silu(mm(message_ref[...].astype(bf16), weight_all_ref[middle_at])).astype(bf16)
    out_ref[...] = mm(middle, weight_all_ref[output_at])


def phase_rows(wave_ref, x, y, z, put):
    waves = wave_ref.shape[1]
    step = 64
    for first in range(0, waves, step):
        part = slice(first, first + step)
        kx, ky, kz = [
            jnp.concatenate([wave_ref[a, part, :]] * (x.shape[1] // LANES), axis=1) for a in range(3)
        ]
        angle = kx * x + ky * y + kz * z
        rest = angle - jnp.round(angle)
        square = rest * rest
        put(first, power_sum(COS_TURN, square).astype(bf16))
        put(waves + first, (power_sum(SIN_TURN, square) * rest).astype(bf16))


def wave_columns(wave_ref, table_ref):
    waves = wave_ref.shape[1]
    eye = identity(LANES, LANES)
    numbers = jnp.concatenate([wave_ref[...].astype(f32), jnp.zeros((5, waves), f32)], axis=0).astype(bf16)
    for first in range(0, waves, LANES):
        turned = mm_nt(eye, numbers[:, first : first + LANES])
        for a in range(3):
            table_ref[a, first : first + LANES, :] = jnp.broadcast_to(turned[:, a : a + 1], (LANES, LANES))


def ewald_kernel(
    depth,
    total_atoms,
    index,
    keep,
    reuse,
    *refs,
):
    refs = list(refs)
    if reuse:
        base_ref = refs.pop(0)
        own_phase_ref, kept_ref = refs.pop(0), refs.pop(0)
        wave_ref, screen_ref, state_ref, own_ref, conv_ref, charge_ref, update_ref, out_ref = refs[:8]
        refs = refs[8:]
        planes, columns = state_ref.shape[0], state_ref.shape[1]
    else:
        wave_ref, screen_ref, geo_ref = refs[:3]
        refs = refs[3:]
        state_ref = geo_ref if index == 0 else refs.pop(0)
        own_ref, conv_ref, charge_ref, update_ref, out_ref = refs[:5]
        refs = refs[5:]
        if keep:
            base_out_ref, own_phase_ref, kept_ref = refs[:3]
            refs = refs[3:]
        else:
            own_phase_ref, base_out_ref = refs[:2]
            refs = refs[2:]
        base_ref, rows_ref, turned_ref, live_ref, packed_geo_ref, spot_ref, base_sem = refs[:7]
        refs = refs[7:]
        planes, columns = geo_ref.shape[0], geo_ref.shape[1]
    table_ref, phase_ref, factor_ref, damp_ref, packed_ref, tile_ref, phase_sem = refs
    atoms, channels = own_ref.shape
    slots = atoms // depth
    waves = wave_ref.shape[1]
    everyone = planes * columns
    wave_columns(wave_ref, table_ref)

    if not reuse:
        row = iota((3, 1), 0)
        unit = jnp.where(row == 0, 1.0 / planes, jnp.where(row == 1, 1.0 / columns, 1.0 / depth))

        def plane_rows(s, carry):
            spots, lives = [], []
            for t in range(columns):
                known = geo_ref[s, t, atoms : atoms + GEO, :].astype(f32)
                offset = (known[0:3] + known[MID : MID + 3]) + known[LOW : LOW + 3]
                spots += [(known[SPOT : SPOT + 3] + offset) * unit, jnp.zeros((1, atoms), f32)]
                lives.append(known[LIVE : LIVE + 1])
            tall = 4 * columns
            rows_ref[pl.ds(pl.multiple_of(s * tall, tall), tall), :] = jnp.concatenate(spots, axis=0)
            live_ref[pl.ds(pl.multiple_of(s * columns, columns), columns), :] = jnp.concatenate(lives, axis=0)
            return carry

        lax.fori_loop(0, planes, plane_rows, 0, unroll=4 if planes % 4 == 0 else 1)
        live = live_ref[...]
        before = (iota((atoms, atoms), 0) < iota((atoms, atoms), 1)).astype(f32).astype(bf16)
        live_b = live.astype(bf16)
        number = mm(live_b, jnp.ones((atoms, atoms), bf16))
        above = (iota((everyone, everyone), 1) < iota((everyone, everyone), 0)).astype(f32).astype(bf16)
        start = mm(above, number.astype(bf16))
        base_out_ref[0:everyone, :] = (mm(live_b, before) + start).astype(jnp.int32)
        last = (number + start)[everyone - 1 : everyone, :].astype(jnp.int32)
        base_out_ref[everyone : everyone + 8, :] = jnp.broadcast_to(last, (8, atoms))
        base_copy = pltpu.make_async_copy(base_out_ref, base_ref, base_sem)
        base_copy.start()
        for b in range(turned_ref.shape[0]):
            turned_ref[b] = rows_ref[b * LANES : (b + 1) * LANES, :].T
        own_rows = geo_ref[0, 0, atoms : atoms + GEO, :].astype(f32)
        offset = (own_rows[0:3] + own_rows[MID : MID + 3]) + own_rows[LOW : LOW + 3]
        own_spot = (own_rows[SPOT : SPOT + 3] + offset) * unit
        own_live = own_rows[LIVE : LIVE + 1].astype(bf16)

        def put_own(first, value):
            own_phase_ref[first : first + value.shape[0], :] = value * own_live

        phase_rows(table_ref, own_spot[0:1], own_spot[1:2], own_spot[2:3], put_own)

    full_turn = 6.283185307179586
    kx = table_ref[0] * (full_turn / planes)
    ky = table_ref[1] * (full_turn / columns)
    kz = table_ref[2] * (full_turn / depth)
    norm = 2.0 / math.sqrt(total_atoms)
    damp_ref[...] = norm * jnp.exp(-(kx * kx + ky * ky + kz * kz) / (4.0 * screen_ref[index : index + 1, :]))
    factor_ref[...] = jnp.zeros_like(factor_ref)
    if not reuse:
        base_copy.wait()
    total = base_ref[everyone, 0]
    pairs = (total + (CHUNK - 1)) // CHUNK

    def phase_copy(p, slot):
        if reuse:
            return pltpu.make_async_copy(kept_ref.at[p], phase_ref.at[slot], phase_sem.at[slot])
        return pltpu.make_async_copy(phase_ref.at[slot], kept_ref.at[p], phase_sem.at[slot])

    if reuse:
        for p in range(AHEAD - 1):

            @pl.when(p < pairs)
            def _(p=p):
                phase_copy(p, p).start()

    def pack_step(s, carry):
        for t in range(columns):
            c = s * columns + t
            for cell in range(depth):
                rows = pl.ds(base_ref[c, cell * slots], slots)
                part = slice(cell * slots, (cell + 1) * slots)
                packed_ref[rows, :] = state_ref[s, t, part, :].astype(f32)
                if not reuse:
                    spread = LANES // 4
                    mine = iota((slots, LANES), 1) // 4 == lax.rem(c, spread)
                    packed_geo_ref[rows, :] = jnp.where(mine, turned_ref[c // spread, part, :], 0.0)
        return carry

    lax.fori_loop(0, planes, pack_step, 0, unroll=2 if planes % 2 == 0 else 1)

    def prepare(p):
        rows = pl.ds(pl.multiple_of(p * CHUNK, CHUNK), CHUNK)
        slot = lax.rem(p, 2)
        valid = iota((CHUNK, channels), 0) + p * CHUNK < total
        picked = jnp.where(valid, packed_ref[rows, :], 0.0).astype(bf16)
        tile_ref[slot] = mm(picked, charge_ref[index]).astype(bf16)
        if not reuse:
            known = packed_geo_ref[rows, :].T
            known = jnp.sum(known.reshape(LANES // 8, 8, CHUNK), axis=0)
            known = known[0:4] + known[4:8]
            valid = iota((4, CHUNK), 1) + p * CHUNK < total
            spot_ref[slot, 0:4, :] = jnp.where(valid, known, 0.0)

    prepare(jnp.int32(0))

    def pair_step(p, carry):
        slot = lax.rem(p, 2)
        charge = tile_ref[slot]
        if reuse:

            ring = lax.rem(p, AHEAD)

            @pl.when(p + AHEAD - 1 < pairs)
            def _():
                phase_copy(p + AHEAD - 1, lax.rem(p + AHEAD - 1, AHEAD)).start()

            phase_copy(p, ring).wait()
        else:
            ring = slot
            spot = spot_ref[slot]
            if keep:

                @pl.when(p >= 2)
                def _():
                    phase_copy(p - 2, slot).wait()

            def put(first, value):
                phase_ref[slot, first : first + value.shape[0], :] = value

            phase_rows(table_ref, spot[0:1], spot[1:2], spot[2:3], put)
        factor_ref[...] += mm(phase_ref[ring], charge)
        if keep and not reuse:
            phase_copy(p, slot).start()
        prepare(jnp.minimum(p + 1, pairs - 1))
        return carry

    lax.fori_loop(0, pairs, pair_step, 0)
    for side in range(2):
        part = slice(side * waves, (side + 1) * waves)
        factor_ref[part, :] = factor_ref[part, :] * damp_ref[...]
    damped = factor_ref[...].astype(bf16)
    field = mm_tn(own_phase_ref[...], damped)
    field = (field * (1.0 / math.sqrt(waves))).astype(bf16)
    ewald = silu(mm(field, update_ref[index]))
    out_ref[...] = (own_ref[...].astype(f32) + ewald + conv_ref[...]).astype(bf16)
    if keep and not reuse:

        @pl.when(pairs >= 2)
        def _():
            phase_copy(pairs - 2, lax.rem(pairs, 2)).wait()

        phase_copy(pairs - 1, lax.rem(pairs + 1, 2)).wait()


def gathered(rows, axis):
    size = lax.axis_size(axis)
    moved = [rows]
    near = [1, size - 1]
    for shift in near + list(range(2, size - 1)):
        moved.append(lax.ppermute(rows, axis, [(i, (i + shift) % size) for i in range(size)]))
    order = [0] + near + list(range(2, size - 1))
    return [moved[order.index(i)] for i in range(size)]


def shards(
    features,
    offsets,
    counts,
    wave_index,
    screening,
    charge_weight,
    ewald_weight,
    input_weight,
    filter_weight,
    middle_weight,
    output_weight,
):
    depth = counts.shape[2]
    atoms, channels = features.shape[2:]
    slots = atoms // depth
    nx = lax.axis_size("gx")
    ny = lax.axis_size("gy")
    waves = wave_index.shape[1]
    assert atoms == channels == filter_weight.shape[1] == LANES and waves % 64 == 0
    state = features.reshape(atoms, channels)
    weights = jnp.concatenate([input_weight, filter_weight, middle_weight, output_weight], axis=0)
    payload = pl.pallas_call(
        pack_kernel,
        out_shape=jax.ShapeDtypeStruct((atoms + GEO, channels), bf16),
        in_specs=[smem(), vmem(), vmem()],
        out_specs=vmem(),
        compiler_params=pltpu.CompilerParams(vmem_limit_bytes=4 * 2**20),
        name="pack",
    )(counts, features, offsets.reshape(3, atoms))

    rows_of = (0, 1, ny - 1)
    columns = 3 * len(rows_of)
    tall = columns + -columns % 8
    count = filter_weight.shape[1]

    def spread_out(rows):
        return gathered(jnp.stack(gathered(rows, "gy")), "gx")

    conv_call = lambda index: pl.pallas_call(
        functools.partial(conv_kernel, depth, slots, nx, ny, rows_of, index),
        out_shape=jax.ShapeDtypeStruct((atoms, channels), f32),
        in_specs=[vmem() for _ in range(7)],
        out_specs=vmem(),
        scratch_shapes=[
            pltpu.VMEM((columns * atoms, 2 * channels), bf16),
            pltpu.VMEM((depth * tall, atoms), f32),
            pltpu.VMEM((atoms, WIDE), f32),
            pltpu.VMEM((atoms, WIDE), f32),
            pltpu.VMEM((GROUP * count, WIDE), bf16),
            pltpu.VMEM((count, channels), f32),
            pltpu.VMEM((count, WIDE), f32),
            pltpu.VMEM((atoms, channels), f32),
            pltpu.VMEM((depth, WIDE, channels), bf16),
            pltpu.VMEM((atoms, LANES), f32),
            pltpu.SMEM((depth,), jnp.int32),
        ],
        compiler_params=pltpu.CompilerParams(vmem_limit_bytes=16 * 2**20),
        cost_estimate=pl.CostEstimate(flops=40_000_000_000, transcendentals=0, bytes_accessed=2_000_000),
        name="conv",
    )
    everyone = nx * ny
    most_pairs = -(-everyone * atoms // CHUNK)
    keep = most_pairs * 2 * waves * CHUNK * 2 <= 16 * 2**20
    most_rows = most_pairs * CHUNK + slots
    room = min((12 + everyone // 3) * 2**20, 60 * 2**20)

    def ewald_call(index, *operands):
        reuse = keep and index > 0
        geometry = [] if reuse else [
            pltpu.SMEM((everyone + 8, atoms), jnp.int32),
            pltpu.VMEM((everyone * 4, LANES), f32),
            pltpu.VMEM((everyone * 4 // LANES, LANES, LANES), f32),
            pltpu.VMEM((everyone, atoms), f32),
            pltpu.VMEM((most_rows, LANES), f32),
            pltpu.VMEM((2, 8, CHUNK), f32),
            pltpu.SemaphoreType.DMA,
        ]
        own_phase, base = ((2 * waves, LANES), bf16), ((everyone + 8, atoms), jnp.int32)
        out_shape = [jax.ShapeDtypeStruct((atoms, channels), bf16)]
        out_specs = [vmem()]
        in_specs = [vmem() for _ in operands]
        hbm = pl.BlockSpec(memory_space=pl.ANY)
        if reuse:
            in_specs[0], in_specs[2] = smem(), hbm
        elif keep:
            out_shape += [jax.ShapeDtypeStruct(*base[:2]), jax.ShapeDtypeStruct(*own_phase[:2])]
            out_shape.append(jax.ShapeDtypeStruct((most_pairs, 2 * waves, CHUNK), bf16))
            out_specs += [vmem(), vmem(), hbm]
        else:
            geometry = [pltpu.VMEM(*own_phase), pltpu.VMEM(*base)] + geometry
        return pl.pallas_call(
            functools.partial(ewald_kernel, depth, everyone * atoms, index, keep, reuse),
            out_shape=out_shape,
            in_specs=in_specs,
            out_specs=out_specs,
            scratch_shapes=geometry
            + [
                pltpu.VMEM((3, waves, LANES), f32),
                pltpu.VMEM((AHEAD if reuse else 2, 2 * waves, CHUNK), bf16),
                pltpu.VMEM((2 * waves, channels), f32),
                pltpu.VMEM((waves, channels), f32),
                pltpu.VMEM((most_rows, channels), f32),
                pltpu.VMEM((2, CHUNK, channels), bf16),
                pltpu.SemaphoreType.DMA((AHEAD if reuse else 2,)),
            ],
            compiler_params=pltpu.CompilerParams(vmem_limit_bytes=room),
            cost_estimate=pl.CostEstimate(flops=30_000_000_000, transcendentals=0, bytes_accessed=4_000_000),
            name="ewald",
        )(*operands)

    geo_planes = spread_out(payload)
    geo_all = jnp.stack(geo_planes)
    state_planes, state_all = geo_planes, geo_all
    for block in range(2):
        if block:
            state_planes = spread_out(state)
            state_all = jnp.stack(state_planes)
        conv = conv_call(block)(
            geo_planes[0],
            geo_planes[1],
            geo_planes[nx - 1],
            state_planes[0],
            state_planes[1],
            state_planes[nx - 1],
            weights,
        )
        common = (state, conv, charge_weight, ewald_weight)
        if block == 0:
            state, *kept = ewald_call(block, wave_index, screening, geo_all, *common)
        elif keep:
            (state,) = ewald_call(block, *kept, wave_index, screening, state_all, *common)
        else:
            (state,) = ewald_call(block, wave_index, screening, geo_all, state_all, *common)
    return state.reshape(features.shape)


def solution(mesh):
    in_specs = (
        P("gx", "gy", None, None),
        P("gx", "gy", None, None),
        P("gx", "gy", None),
        P(),
        P(),
        P(),
        P(),
        P(),
        P(),
        P(),
        P(),
    )
    out_specs = P("gx", "gy", None, None)
    return jax.shard_map(shards, mesh=mesh, in_specs=in_specs, out_specs=out_specs, check_vma=False)
```
